32 devices in a mesh: pr: 8 (over y, x, core), pc: 4 (over z).
Axes of the slice: x: 2, y: 2, z: 4, core: 2. Of those that a mesh axis runs over, the one named last changes fastest.
Arguments:
- pair_array: bfloat16 [256, 256, 128], P('pr', 'pc'), may hold values from -6 to 6
- left_weight: bfloat16 [128, 128], replicated, may hold values from -0.5 to 0.5
- right_weight: bfloat16 [128, 128], replicated, may hold values from -0.5 to 0.5
- left_gate: bfloat16 [128, 128], replicated, may hold values from -0.5 to 0.5
- right_gate: bfloat16 [128, 128], replicated, may hold values from -0.5 to 0.5
- mid_gain: float32 [128], replicated, may hold values from 0.25 to 1.75
- out_weight: bfloat16 [128, 128], replicated, may hold values from -0.5 to 0.5
- out_gate: bfloat16 [128, 128], replicated, may hold values from -0.5 to 0.5
Outputs:
- pair_update: bfloat16 [256, 256, 128], P('pr', 'pc')
The draws below stay inside these ranges and needn't reach their ends.
All inputs are finite; a program needn't handle non-finite values.
Results may differ from the reference program's by a relative error of at most 0.012.
Values may be sent and summed in bfloat16 or wider, within the bound.
No kernel may reach another device: no remote copies, remote signals or barrier semaphores. Data moves between devices by JAX's collectives and lax.ppermute only.
A program may use at most 128 MiB of HBM per device.

```python
import jax
import jax.numpy as jnp
from jax import lax

RESIDUES = 256
PAIR_WIDTH = 128
MIX_WIDTH = 128


def shard_levels(rng, extent, pieces, least, largest):
    loudness = 1.0
    for axis_at, parts in pieces:
        draws = jax.random.uniform(jax.random.fold_in(jax.random.fold_in(rng, 6), axis_at), (parts,), jnp.float32, least / len(pieces), largest / len(pieces))
        loudness = loudness * jnp.repeat(jnp.exp(draws), extent[axis_at] // parts).reshape((-1,) + (1,) * (len(extent) - 1 - axis_at))
    return loudness


def bell_draw(key, shape, scale, reach, pieces=(), dtype=jnp.bfloat16):
    entries = jax.random.normal(key, shape, jnp.float32) * scale
    if len(pieces) > 0:
        entries = shard_levels(key, shape, pieces, -0.22, 0.18) * entries
    return jnp.clip(entries, min=-reach, max=reach).astype(dtype)


def setup_inputs(seed: int = 0) -> dict:
    keys = jax.random.split(jax.random.key(seed), 9)
    pair_array = bell_draw(keys[0], (RESIDUES, RESIDUES, PAIR_WIDTH), 1.0, 6.0, ((0, 8), (1, 4)))
    left_weight = bell_draw(keys[1], (PAIR_WIDTH, MIX_WIDTH), PAIR_WIDTH ** -0.5, 0.5)
    right_weight = bell_draw(keys[2], (PAIR_WIDTH, MIX_WIDTH), PAIR_WIDTH ** -0.5, 0.5)
    left_gate = bell_draw(keys[3], (PAIR_WIDTH, MIX_WIDTH), PAIR_WIDTH ** -0.5, 0.5)
    right_gate = bell_draw(keys[4], (PAIR_WIDTH, MIX_WIDTH), PAIR_WIDTH ** -0.5, 0.5)
    mid_gain = jnp.clip(1.0 + 0.15 * jax.random.normal(keys[5], (MIX_WIDTH,), jnp.float32), 0.25, 1.75)
    out_weight = bell_draw(keys[6], (MIX_WIDTH, PAIR_WIDTH), MIX_WIDTH ** -0.5, 0.5)
    out_gate = bell_draw(keys[7], (PAIR_WIDTH, PAIR_WIDTH), PAIR_WIDTH ** -0.5, 0.5)
    return {"pair_array": pair_array, "left_weight": left_weight, "right_weight": right_weight, "left_gate": left_gate, "right_gate": right_gate, "mid_gain": mid_gain, "out_weight": out_weight, "out_gate": out_gate}


def unit_channels(values, channel_gain):
    centred = values - lax.optimization_barrier(jnp.mean(values, axis=-1, keepdims=True))
    return centred * lax.rsqrt(lax.optimization_barrier(jnp.mean(centred * centred, axis=-1, keepdims=True)) + 1e-05) * channel_gain

def make_factors(pair_in, left_weight, right_weight, left_gate, right_gate):
    ready = pair_in
    left = jnp.einsum('ijc,cd->ijd', ready.astype(jnp.float32), left_weight.astype(jnp.float32))
    left = left * jax.nn.sigmoid(jnp.einsum('ijc,cd->ijd', ready.astype(jnp.float32), left_gate.astype(jnp.float32)))
    right = jnp.einsum('ijc,cd->ijd', ready.astype(jnp.float32), right_weight.astype(jnp.float32))
    right = right * jax.nn.sigmoid(jnp.einsum('ijc,cd->ijd', ready.astype(jnp.float32), right_gate.astype(jnp.float32)))
    return (ready, left.astype(jnp.bfloat16), right.astype(jnp.bfloat16))

def to_pair(mixed, ready, mid_gain, out_weight, out_gate):
    scaled = unit_channels(mixed.astype(jnp.float32), mid_gain).astype(jnp.bfloat16)
    scaled = lax.optimization_barrier(scaled)
    gate = jax.nn.sigmoid(jnp.einsum('ijc,cd->ijd', ready.astype(jnp.float32), out_gate.astype(jnp.float32)))
    return (jnp.einsum('ijd,dc->ijc', scaled.astype(jnp.float32), out_weight.astype(jnp.float32)) * gate).astype(jnp.bfloat16)

def reference(pair_array, left_weight, right_weight, left_gate, right_gate, mid_gain, out_weight, out_gate):
    ready, left, right = make_factors(pair_array, left_weight, right_weight, left_gate, right_gate)
    left, right = lax.optimization_barrier((left, right))

    def one_channel(pair_of):
        return (jnp.dot(pair_of[0].T, pair_of[1], preferred_element_type=jnp.float32) * RESIDUES ** (-0.5)).astype(jnp.bfloat16)
    mixed = jnp.moveaxis(lax.map(one_channel, (jnp.moveaxis(left, -1, 0), jnp.moveaxis(right, -1, 0))), 0, -1)
    mixed = lax.optimization_barrier(mixed)
    return to_pair(mixed, ready, mid_gain, out_weight, out_gate)
```

```python
import functools

import jax
import jax.numpy as jnp
from jax import lax
from jax.experimental import pallas as pl
from jax.experimental.pallas import tpu as pltpu
from jax.sharding import PartitionSpec as P

F32, BF16 = jnp.float32, jnp.bfloat16
LANES = 128
VMEM = pl.BlockSpec(memory_space=pltpu.VMEM)


def dot(a, b, over_a, over_b):
    return lax.dot_general(a, b, (((over_a,), (over_b,)), ((), ())), preferred_element_type=F32)


def logistic(v):
    return 0.5 * jnp.tanh(0.5 * v) + 0.5


def factors_kernel(x_ref, lw_ref, lg_ref, rw_ref, rg_ref, out_ref, left_ref, right_ref):
    width = lw_ref.shape[1]
    rows = x_ref.shape[0] // LANES
    weights = jnp.concatenate(
        [w[...].astype(F32).T.astype(BF16) for w in (lw_ref, lg_ref, rw_ref, rg_ref)], axis=0
    )

    def chunk(s, _):
        x = x_ref[pl.ds(pl.multiple_of(s * 2 * LANES, 2 * LANES), 2 * LANES), :]
        y = dot(weights, x, 1, 1)
        left = y[:width] * logistic(y[width : 2 * width])
        right = y[2 * width : 3 * width] * logistic(y[3 * width :])
        for h in range(2):
            at = pl.ds(2 * s + h, width, stride=rows)
            left_ref[at, :] = left[:, h * LANES : (h + 1) * LANES]
            right_ref[at, :] = right[:, h * LANES : (h + 1) * LANES]
        return 0

    lax.fori_loop(0, rows // 2, chunk, 0, unroll=2)
    shape = (out_ref.shape[0],) + out_ref.shape[2:]
    out_ref[:, 0] = left_ref[...].astype(BF16).reshape(shape)
    out_ref[:, 1] = right_ref[...].astype(BF16).reshape(shape)


def lines_of(ref, ch, fold):
    pr, pc = ref.shape[:2]
    width = LANES // fold
    blocks = [jnp.concatenate([ref[p, c, 0, ch] for p in range(pr)], axis=0) for c in range(pc)]
    return [
        jnp.concatenate([b[:, e * width : (e + 1) * width] for b in blocks], axis=1)
        for e in range(fold)
    ]


def product_kernel(fold, scale, left_ref, right_ref, out_ref):
    rows_of, pc, channels, rows = out_ref.shape[:4]
    width = LANES // fold
    for ch in range(channels):
        left = lines_of(left_ref, ch, fold)
        right = lines_of(right_ref, ch, fold)
        mixed = sum(dot(a, b, 0, 0) for a, b in zip(left, right)) * scale
        for p in range(rows_of):
            at = p * rows * fold
            for c in range(pc):
                block = [
                    mixed[at + f * rows : at + (f + 1) * rows, c * width : (c + 1) * width]
                    for f in range(fold)
                ]
                block = block[0] if fold == 1 else jnp.concatenate(block, axis=1)
                out_ref[p, c, ch] = block.astype(BF16)


def pair_kernel(fold, x_ref, mixed_ref, gain_ref, ow_ref, og_ref, out_ref, held_ref):
    depth, rows = mixed_ref.shape[:2]
    width = LANES // fold
    mixed = mixed_ref[...].astype(F32)
    held_ref[...] = mixed.reshape(depth * rows, LANES)
    mean = jnp.sum(mixed, axis=0) * (1.0 / depth)
    centred = mixed - mean[None]
    root = lax.rsqrt(jnp.sum(centred * centred, axis=0) * (1.0 / depth) + 1e-05)
    gain = jnp.broadcast_to(gain_ref[...], (LANES, depth)).T
    weight, gates = ow_ref[...], og_ref[...]
    for s in range(rows):
        v = held_ref[pl.ds(s, depth, stride=rows), :]
        scaled = ((v - mean[s : s + 1]) * root[s : s + 1] * gain).astype(BF16)
        x = jnp.concatenate([x_ref[f * rows + s] for f in range(fold)], axis=0)
        y = dot(scaled, weight, 0, 0) * logistic(dot(x, gates, 1, 0))
        for f in range(fold):
            out_ref[f * rows + s] = y[f * width : (f + 1) * width].astype(BF16)


def on_device(
    pair_array, left_weight, right_weight, left_gate, right_gate, mid_gain, out_weight, out_gate
):
    pr, pc = lax.axis_size("pr"), lax.axis_size("pc")
    n = pr * pc
    lines, ours, depth = pair_array.shape
    mix = left_weight.shape[1]
    count = lines * pr
    fold = max(1, LANES // ours)
    rows = lines * ours // LANES
    channels = mix // n
    factors = pl.pallas_call(
        factors_kernel,
        out_shape=jax.ShapeDtypeStruct((n, 2, channels * rows, LANES), BF16),
        in_specs=[VMEM] * 5,
        out_specs=VMEM,
        scratch_shapes=[pltpu.VMEM((mix * rows, LANES), F32)] * 2,
        compiler_params=pltpu.CompilerParams(vmem_limit_bytes=48 << 20),
        name="factors",
    )(
        pair_array.reshape(lines * ours, depth), left_weight, left_gate, right_weight, right_gate
    )
    factors = lax.all_to_all(factors, ("pr", "pc"), 0, 0, tiled=True)
    factors = factors.reshape(pr, pc, 2, channels, rows, LANES)
    whole = count * count * 4 * channels <= (2 << 20)
    at_once, blocks = (channels, pc) if whole else (1, 1)
    mixed = pl.pallas_call(
        functools.partial(product_kernel, fold, count ** (-0.5)),
        grid=(channels // at_once, pc // blocks),
        out_shape=jax.ShapeDtypeStruct((pr, pc, channels, rows, LANES), BF16),
        in_specs=[
            pl.BlockSpec((pr, blocks, 1, at_once, rows, LANES), lambda h, c: (0, c, 0, h, 0, 0)),
            pl.BlockSpec((pr, pc, 1, at_once, rows, LANES), lambda h, c: (0, 0, 1, h, 0, 0)),
        ],
        out_specs=pl.BlockSpec(
            (pr * blocks // pc, pc, at_once, rows, LANES), lambda h, c: (c, 0, h, 0, 0)
        ),
        compiler_params=pltpu.CompilerParams(vmem_limit_bytes=48 << 20),
        name="product",
    )(factors, factors)
    mixed = mixed.reshape(n, channels * rows, LANES)
    mixed = lax.all_to_all(mixed, ("pr", "pc"), 0, 0, tiled=True)
    return pl.pallas_call(
        functools.partial(pair_kernel, fold),
        out_shape=jax.ShapeDtypeStruct(pair_array.shape, BF16),
        in_specs=[VMEM] * 5,
        out_specs=VMEM,
        scratch_shapes=[pltpu.VMEM((mix * rows, LANES), F32)],
        compiler_params=pltpu.CompilerParams(vmem_limit_bytes=48 << 20),
        name="pair",
    )(pair_array, mixed.reshape(mix, rows, LANES), mid_gain.reshape(1, mix), out_weight, out_gate)


def solution(mesh):
    return jax.shard_map(
        on_device,
        mesh=mesh,
        in_specs=(P("pr", "pc", None), P(), P(), P(), P(), P(), P(), P()),
        out_specs=P("pr", "pc", None),
        check_vma=False,
    )
```

```python
import functools

import jax
import jax.numpy as jnp
from jax import lax
from jax.experimental import pallas as pl
from jax.experimental.pallas import tpu as pltpu
from jax.sharding import Mesh, PartitionSpec as P

F32, BF16 = jnp.float32, jnp.bfloat16
LANES = 128
HALF = ("pr", "pl")
ALL = ("pr", "ph", "pl")
VMEM = pl.BlockSpec(memory_space=pltpu.VMEM)
HBM = pl.BlockSpec(memory_space=pltpu.HBM)


def dot(a, b, over_a, over_b):
    return lax.dot_general(a, b, (((over_a,), (over_b,)), ((), ())), preferred_element_type=F32)


def logistic(v):
    return 0.5 * jnp.tanh(0.5 * v) + 0.5


def params(limit=48 << 20):
    return pltpu.CompilerParams(vmem_limit_bytes=limit)


def cost(flops, nbytes):
    return pl.CostEstimate(flops=flops, bytes_accessed=nbytes, transcendentals=0)


def factor_into(held_ref, x_ref, weights):
    width = weights.shape[0] // 2
    rows = held_ref.shape[0] // width
    step = 2 * LANES

    def chunk(s, _):
        x = x_ref[pl.ds(pl.multiple_of(s * step, step), step), :]
        y = dot(weights, x, 1, 1)
        line = y[:width] * logistic(y[width:])
        for h in range(2):
            held_ref[pl.ds(2 * s + h, width, stride=rows), :] = line[:, h * LANES : (h + 1) * LANES]
        return 0

    lax.fori_loop(0, rows // 2, chunk, 0, unroll=2)


def turned(*refs):
    return jnp.concatenate([r[...].astype(F32).T.astype(BF16) for r in refs], axis=0)


def left_kernel(x_hbm, w_hbm, g_hbm, out_ref, held_ref, x_ref, w_ref, g_ref, sems):
    copies = [
        pltpu.make_async_copy(a, b, sems.at[i])
        for i, (a, b) in enumerate(((w_hbm, w_ref), (g_hbm, g_ref), (x_hbm, x_ref)))
    ]
    for copy in copies:
        copy.start()
    for copy in copies[:2]:
        copy.wait()
    weights = turned(w_ref, g_ref)
    copies[2].wait()
    factor_into(held_ref, x_ref, weights)
    pr, ph, pc, size = out_ref.shape[:4]
    lines = held_ref[...].astype(BF16).reshape(pr, pc, size, LANES)
    for h in range(ph):
        out_ref[:, h] = lines


def right_kernel(x_ref, w_ref, g_ref, *rest):
    outs, held_ref = rest[:-1], rest[-1]
    factor_into(held_ref, x_ref, turned(w_ref, g_ref))
    if len(outs) == 1:
        outs[0][...] = held_ref[...].astype(BF16).reshape(outs[0].shape)
    else:
        me = lax.axis_index(HALF)
        size = outs[0].shape[0]
        for s, out in enumerate(outs):
            at = pl.multiple_of((me ^ s) * size, size)
            out[...] = held_ref[pl.ds(at, size), :].astype(BF16)


def gate_kernel(x_ref, og_ref, gain_ref, out_ref, gains_ref):
    out_ref[...] = logistic(dot(x_ref[...], og_ref[...], 1, 0))
    gains_ref[...] = jnp.broadcast_to(gain_ref[...], (LANES, gain_ref.shape[1])).T


def lines_of(get, pr, pc, fold):
    width = LANES // fold
    blocks = [jnp.concatenate([get(p, c) for p in range(pr)], axis=0) for c in range(pc)]
    parts = [
        jnp.concatenate([b[:, e * width : (e + 1) * width] for b in blocks], axis=1)
        for e in range(fold)
    ]
    return parts[0] if fold == 1 else jnp.concatenate(parts, axis=0)


def product_kernel(fold, scale, left_ref, *rest):
    rights, out_ref = rest[: len(rest) - 2], rest[-2]
    held = rest[-1]
    rows_of, pc, channels, rows = out_ref.shape[:4]
    pr, blocks = left_ref.shape[:2]
    width = LANES // fold
    if len(rights) > 1:
        me = lax.axis_index(HALF)
        for s, right in enumerate(rights):
            held[me ^ s] = right[...]

    for ch in range(channels):
        left = lines_of(lambda p, c: left_ref[p, c, ch], pr, blocks, fold)
        if len(rights) > 1:
            at = slice(ch * rows, (ch + 1) * rows)
            right = lines_of(lambda p, c: held[p * pc + c, at, :], pr, pc, fold)
        else:
            right = lines_of(lambda p, c: rights[0][p, c, ch], pr, pc, fold)
        mixed = dot(left, right, 0, 0) * scale
        for p in range(rows_of):
            at = p * rows * fold
            for c in range(pc):
                block = [
                    mixed[at + f * rows : at + (f + 1) * rows, c * width : (c + 1) * width]
                    for f in range(fold)
                ]
                block = block[0] if fold == 1 else jnp.concatenate(block, axis=1)
                out_ref[p, c, ch] = block.astype(BF16)


def pair_kernel(fold, mixed_ref, gate_ref, gains_ref, ow_ref, out_ref, held_ref):
    depth, rows = mixed_ref.shape[:2]
    width = LANES // fold
    mixed = mixed_ref[...].astype(F32)
    held_ref[...] = mixed.reshape(depth * rows, LANES)
    mean = jnp.sum(mixed, axis=0) * (1.0 / depth)
    centred = mixed - mean[None]
    root = lax.rsqrt(jnp.sum(centred * centred, axis=0) * (1.0 / depth) + 1e-05)
    gain, weight = gains_ref[...], ow_ref[...]
    for s in range(rows):
        v = held_ref[pl.ds(s, depth, stride=rows), :]
        scaled = ((v - mean[s : s + 1]) * root[s : s + 1] * gain).astype(BF16)
        y = dot(scaled, weight, 0, 0)
        for f in range(fold):
            at = f * rows + s
            out_ref[at] = (y[f * width : (f + 1) * width] * gate_ref[at]).astype(BF16)


def on_device(
    pair_array, left_weight, right_weight, left_gate, right_gate, mid_gain, out_weight, out_gate
):
    pr, ph, pc = lax.axis_size("pr"), lax.axis_size("ph"), lax.axis_size("pl")
    m = pr * pc
    lines, ours, depth = pair_array.shape
    mix = left_weight.shape[1]
    count = lines * pr
    fold = max(1, LANES // ours)
    rows = lines * ours // LANES
    channels = mix // m
    size = channels * rows
    hops = m <= 16 and m & (m - 1) == 0
    flat = pair_array.reshape(lines * ours, depth)
    flops = 4 * lines * ours * depth * mix

    copied = [pltpu.VMEM(a.shape, BF16) for a in (flat, left_weight, left_gate)]
    copied.append(pltpu.SemaphoreType.DMA((3,)))

    def factor(kernel, out_shape, w, g, name):
        first = name == "left"
        return pl.pallas_call(
            kernel,
            out_shape=out_shape,
            in_specs=[HBM if first else VMEM] * 3,
            out_specs=jax.tree.map(lambda _: VMEM, out_shape),
            scratch_shapes=[pltpu.VMEM((mix * rows, LANES), F32)] + (copied if first else []),
            compiler_params=params(67043328 if first else 48 << 20),
            cost_estimate=cost(flops, 4 * flat.size),
            name=name,
        )(flat, w, g)

    left = factor(
        left_kernel,
        jax.ShapeDtypeStruct((pr, ph, pc, size, LANES), BF16),
        left_weight,
        left_gate,
        "left",
    )
    left = lax.all_to_all(left.reshape(pr * ph * pc, size, LANES), ALL, 0, 0, tiled=True)
    left = left.reshape(pr, ph * pc, channels, rows, LANES)

    block = jax.ShapeDtypeStruct((size, LANES), BF16)
    if hops:
        right = factor(right_kernel, [block] * m, right_weight, right_gate, "right")
        right = [right[0]] + [
            lax.ppermute(right[s], HALF, [(i, i ^ s) for i in range(m)]) for s in range(1, m)
        ]
    else:
        whole = jax.ShapeDtypeStruct((m, size, LANES), BF16)
        right = factor(right_kernel, whole, right_weight, right_gate, "right")
        right = lax.all_to_all(right, HALF, 0, 0, tiled=True)
        right = [right.reshape(pr, pc, channels, rows, LANES)]

    gate, gains = pl.pallas_call(
        gate_kernel,
        out_shape=[
            jax.ShapeDtypeStruct((lines * ours, depth), F32),
            jax.ShapeDtypeStruct((mix, LANES), F32),
        ],
        in_specs=[VMEM] * 3,
        out_specs=[VMEM] * 2,
        compiler_params=params(),
        cost_estimate=cost(flops // 2, 6 * flat.size),
        name="gate",
    )(flat, out_gate, mid_gain.reshape(1, mix))

    if hops:
        at_once, blocks = channels, ph * pc
        right_specs = [pl.BlockSpec((size, LANES), lambda h, c: (0, 0))] * m
        held = pltpu.VMEM((m, size, LANES), BF16)
    else:
        at_once, blocks = 1, 1
        right_specs = [
            pl.BlockSpec((pr, pc, at_once, rows, LANES), lambda h, c: (0, 0, h, 0, 0))
        ]
        held = pltpu.VMEM((8, LANES), BF16)
    mixed = pl.pallas_call(
        functools.partial(product_kernel, fold, count ** (-0.5)),
        grid=(channels // at_once, ph * pc // blocks),
        out_shape=jax.ShapeDtypeStruct((pr, pc, channels, rows, LANES), BF16),
        in_specs=[
            pl.BlockSpec((pr, blocks, at_once, rows, LANES), lambda h, c: (0, c, h, 0, 0)),
            *right_specs,
        ],
        out_specs=pl.BlockSpec(
            (pr * blocks // (ph * pc), pc, at_once, rows, LANES), lambda h, c: (c, 0, h, 0, 0)
        ),
        scratch_shapes=[held],
        compiler_params=params(),
        cost_estimate=cost(2 * count * count * ours * pc * channels, 8 * flat.size),
        name="product",
    )(left, *right)
    mixed = lax.all_to_all(mixed.reshape(m, size, LANES), HALF, 0, 0, tiled=True)
    return pl.pallas_call(
        functools.partial(pair_kernel, fold),
        out_shape=jax.ShapeDtypeStruct(pair_array.shape, BF16),
        in_specs=[VMEM] * 4,
        out_specs=VMEM,
        scratch_shapes=[pltpu.VMEM((mix * rows, LANES), F32)],
        compiler_params=params(),
        cost_estimate=cost(flops // 2, 8 * flat.size),
        name="pair",
    )(
        mixed.reshape(mix, rows, LANES),
        gate.reshape(lines, ours, depth),
        gains,
        out_weight,
    )


def solution(mesh):
    sizes = dict(mesh.shape)
    parts = 2 if sizes["pc"] % 2 == 0 else 1
    split = Mesh(mesh.devices.reshape(sizes["pr"], parts, sizes["pc"] // parts), ALL)
    spec = P("pr", ("ph", "pl"), None)
    return jax.shard_map(
        on_device,
        mesh=split,
        in_specs=(spec, P(), P(), P(), P(), P(), P(), P()),
        out_specs=spec,
        check_vma=False,
    )
```

```python
import functools

import jax
import jax.numpy as jnp
from jax import lax
from jax.experimental import pallas as pl
from jax.experimental.pallas import tpu as pltpu
from jax.sharding import Mesh, PartitionSpec as P

F32, BF16 = jnp.float32, jnp.bfloat16
LANES = 128
HALF = ("pr", "pl")
ALL = ("pr", "ph", "pl")
VMEM = pl.BlockSpec(memory_space=pltpu.VMEM)
HBM = pl.BlockSpec(memory_space=pltpu.HBM)


def dot(a, b, over_a, over_b):
    return lax.dot_general(a, b, (((over_a,), (over_b,)), ((), ())), preferred_element_type=F32)


def logistic(v):
    return 0.5 * jnp.tanh(0.5 * v) + 0.5


def params(limit=48 << 20):
    return pltpu.CompilerParams(vmem_limit_bytes=limit)


def cost(flops, nbytes):
    return pl.CostEstimate(flops=flops, bytes_accessed=nbytes, transcendentals=0)


def turned(*refs):
    return jnp.concatenate([r[...].astype(F32).T.astype(BF16) for r in refs], axis=0)


def factor_into(held_ref, rows, weights, take):
    width = weights.shape[0] // 2
    stride = held_ref.shape[0] // width

    def chunk(s, _):
        y = dot(weights, jnp.concatenate([take(2 * s), take(2 * s + 1)], axis=0), 1, 1)
        line = y[:width] * logistic(y[width:])
        for h in range(2):
            held_ref[pl.ds(2 * s + h, width, stride=stride), :] = line[:, h * LANES : (h + 1) * LANES]
        return 0

    lax.fori_loop(0, rows // 2, chunk, 0, unroll=2)
    return held_ref[...].reshape(width, stride, LANES)[:, :rows].astype(BF16)


def left_kernel(x_hbm, w_hbm, g_hbm, out_ref, held_ref, wide_ref, x_ref, w_ref, g_ref, sems):
    copies = [
        pltpu.make_async_copy(a, b, sems.at[i])
        for i, (a, b) in enumerate(((w_hbm, w_ref), (g_hbm, g_ref), (x_hbm, x_ref)))
    ]
    for copy in copies:
        copy.start()
    for copy in copies[:2]:
        copy.wait()
    weights = turned(w_ref, g_ref)
    copies[2].wait()
    lines, ours = x_ref.shape[:2]
    step = ours + 8
    for k in range(lines):
        wide_ref[k * step : k * step + ours, :] = x_ref[k].astype(F32)
    parts = LANES // lines
    rows = ours // parts

    def take(s):
        return jnp.concatenate(
            [wide_ref[pl.ds(q * rows + s, lines, stride=step), :] for q in range(parts)], axis=0
        ).astype(BF16)

    held = factor_into(held_ref, rows, weights, take)
    pr, ph, pc, size = out_ref.shape[:4]
    held = held.reshape(pr, pc, size, LANES)
    for h in range(ph):
        out_ref[:, h] = held


def right_kernel(fold, x_ref, w_ref, g_ref, og_ref, gain_ref, *rest):
    outs, gate_ref, gains_ref, held_ref = rest[:-3], *rest[-3:]
    lines, ours, depth = x_ref.shape
    rows = lines // fold

    def take(s):
        parts = [x_ref[e * rows + s] for e in range(fold)]
        return parts[0] if fold == 1 else jnp.concatenate(parts, axis=0)

    held = factor_into(held_ref, rows, turned(w_ref, g_ref), take)
    if len(outs) == 1:
        outs[0][...] = held.reshape(outs[0].shape)
    else:
        me = lax.axis_index(HALF)
        size = outs[0].shape[0]
        per = size // rows
        stride = held_ref.shape[0] // (per * len(outs))
        for s, out in enumerate(outs):
            at = pl.multiple_of((me ^ s) * (per * stride), per * stride)
            block = held_ref[pl.ds(at, per * stride), :].reshape(per, stride, LANES)
            out[...] = block[:, :rows].reshape(size, LANES).astype(BF16)

    def gate(k, _):
        x = x_ref[pl.ds(k * 2, 2)].reshape(2 * ours, depth)
        gate_ref[pl.ds(k * 2, 2)] = logistic(dot(x, og_ref[...], 1, 0)).reshape(2, ours, depth)
        return 0

    lax.fori_loop(0, lines // 2, gate, 0, unroll=2)
    gains_ref[...] = jnp.broadcast_to(gain_ref[...], (LANES, gain_ref.shape[1])).T


def left_of(ref, ch, lines):
    pr, pc = ref.shape[:2]
    parts = LANES // lines
    return jnp.concatenate(
        [
            jnp.concatenate(
                [ref[p, c, ch, :, q * lines : (q + 1) * lines] for p in range(pr)], axis=1
            )
            for c in range(pc)
            for q in range(parts)
        ],
        axis=0,
    )


def right_of(get, pr, pc, fold):
    width = LANES // fold
    bands = []
    for p in range(pr):
        blocks = [get(p, c) for c in range(pc)]
        for e in range(fold):
            at = slice(e * width, (e + 1) * width)
            bands.append(jnp.concatenate([b[:, at] for b in blocks], axis=1))
    return jnp.concatenate(bands, axis=0)


def product_kernel(fold, scale, left_ref, *rest):
    rights, out_ref, held = rest[:-2], *rest[-2:]
    rows_of, pc, channels, rows = out_ref.shape[:4]
    pr = left_ref.shape[0]
    width = LANES // fold
    if len(rights) > 1:
        me = lax.axis_index(HALF)
        for s, right in enumerate(rights):
            held[me ^ s] = right[...]

    for ch in range(channels):
        left = left_of(left_ref, ch, rows * fold)
        if len(rights) > 1:
            at = slice(ch * rows, (ch + 1) * rows)
            right = right_of(lambda p, c: held[p * pc + c, at, :], pr, pc, fold)
        else:
            right = right_of(lambda p, c: rights[0][p, c, ch], pr, pc, fold)
        mixed = dot(left, right, 1, 0) * scale
        for p in range(rows_of):
            at = p * rows * fold
            for c in range(pc):
                block = [
                    mixed[at + f * rows : at + (f + 1) * rows, c * width : (c + 1) * width]
                    for f in range(fold)
                ]
                block = block[0] if fold == 1 else jnp.concatenate(block, axis=1)
                out_ref[p, c, ch] = block.astype(BF16)


def pair_kernel(fold, mixed_ref, gate_ref, gains_ref, ow_ref, out_ref, held_ref):
    depth, rows = mixed_ref.shape[:2]
    stride = held_ref.shape[1]
    width = LANES // fold
    held_ref[:, :rows] = mixed_ref[...].astype(F32)
    flat_ref = held_ref.reshape(depth * stride, LANES)
    gain, weight = gains_ref[...], ow_ref[...]
    for s in range(rows):
        v = flat_ref[pl.ds(s, depth, stride=stride), :]
        centred = v - jnp.sum(v, axis=0, keepdims=True) * (1.0 / depth)
        spread = jnp.sum(centred * centred, axis=0, keepdims=True) * (1.0 / depth)
        scaled = (centred * lax.rsqrt(spread + 1e-05) * gain).astype(BF16)
        y = dot(scaled, weight, 0, 0)
        for f in range(fold):
            at = f * rows + s
            out_ref[at] = (y[f * width : (f + 1) * width] * gate_ref[at]).astype(BF16)


def on_device(
    pair_array, left_weight, right_weight, left_gate, right_gate, mid_gain, out_weight, out_gate
):
    pr, ph, pc = lax.axis_size("pr"), lax.axis_size("ph"), lax.axis_size("pl")
    m = pr * pc
    lines, ours, depth = pair_array.shape
    mix = left_weight.shape[1]
    count = lines * pr
    fold = max(1, LANES // ours)
    rows = lines * ours // LANES
    channels = mix // m
    size = channels * rows
    hops = m <= 16 and m & (m - 1) == 0
    n_x = pair_array.size
    flops = 4 * lines * ours * depth * mix
    held = pltpu.VMEM((mix * (rows + 8), LANES), F32)

    left = pl.pallas_call(
        left_kernel,
        out_shape=jax.ShapeDtypeStruct((pr, ph, pc, size, LANES), BF16),
        in_specs=[HBM] * 3,
        out_specs=VMEM,
        scratch_shapes=[
            held,
            pltpu.VMEM((lines * (ours + 8), depth), F32),
            *[pltpu.VMEM(a.shape, BF16) for a in (pair_array, left_weight, left_gate)],
            pltpu.SemaphoreType.DMA((3,)),
        ],
        compiler_params=params(67043328),
        cost_estimate=cost(flops, 4 * n_x),
        name="left",
    )(pair_array, left_weight, left_gate)
    left = lax.all_to_all(left.reshape(pr * ph * pc, size, LANES), ALL, 0, 0, tiled=True)
    left = left.reshape(pr, ph * pc, channels, rows, LANES)

    if hops:
        shapes = [jax.ShapeDtypeStruct((size, LANES), BF16)] * m
    else:
        shapes = [jax.ShapeDtypeStruct((m, size, LANES), BF16)]
    shapes += [jax.ShapeDtypeStruct(pair_array.shape, F32), jax.ShapeDtypeStruct((mix, LANES), F32)]
    *right, gate, gains = pl.pallas_call(
        functools.partial(right_kernel, fold),
        out_shape=shapes,
        in_specs=[VMEM] * 5,
        out_specs=[VMEM] * len(shapes),
        scratch_shapes=[held],
        compiler_params=params(),
        cost_estimate=cost(2 * flops, 8 * n_x),
        name="right",
    )(pair_array, right_weight, right_gate, out_gate, mid_gain.reshape(1, mix))
    if hops:
        right[1:] = [
            lax.ppermute(right[s], HALF, [(i, i ^ s) for i in range(m)]) for s in range(1, m)
        ]
    else:
        right = [lax.all_to_all(right[0], HALF, 0, 0, tiled=True)]
        right = [right[0].reshape(pr, pc, channels, rows, LANES)]

    if hops:
        at_once, blocks = channels, ph * pc
        right_specs = [pl.BlockSpec((size, LANES), lambda h, c: (0, 0))] * m
        kept = pltpu.VMEM((m, size, LANES), BF16)
    else:
        at_once, blocks = 1, 1
        right_specs = [
            pl.BlockSpec((pr, pc, at_once, rows, LANES), lambda h, c: (0, 0, h, 0, 0))
        ]
        kept = pltpu.VMEM((8, LANES), BF16)
    mixed = pl.pallas_call(
        functools.partial(product_kernel, fold, count ** (-0.5)),
        grid=(channels // at_once, ph * pc // blocks),
        out_shape=jax.ShapeDtypeStruct((pr, pc, channels, rows, LANES), BF16),
        in_specs=[
            pl.BlockSpec((pr, blocks, at_once, rows, LANES), lambda h, c: (0, c, h, 0, 0)),
            *right_specs,
        ],
        out_specs=pl.BlockSpec(
            (pr * blocks // (ph * pc), pc, at_once, rows, LANES), lambda h, c: (c, 0, h, 0, 0)
        ),
        scratch_shapes=[kept],
        compiler_params=params(),
        cost_estimate=cost(2 * count * count * ours * pc * channels, 8 * n_x),
        name="product",
    )(left, *right)
    mixed = lax.all_to_all(mixed.reshape(m, size, LANES), HALF, 0, 0, tiled=True)
    return pl.pallas_call(
        functools.partial(pair_kernel, fold),
        out_shape=jax.ShapeDtypeStruct(pair_array.shape, BF16),
        in_specs=[VMEM] * 4,
        out_specs=VMEM,
        scratch_shapes=[pltpu.VMEM((mix, rows + 8, LANES), F32)],
        compiler_params=params(),
        cost_estimate=cost(flops // 2, 8 * n_x),
        name="pair",
    )(mixed.reshape(mix, rows, LANES), gate, gains, out_weight)


def solution(mesh):
    sizes = dict(mesh.shape)
    parts = 2 if sizes["pc"] % 2 == 0 else 1
    split = Mesh(mesh.devices.reshape(sizes["pr"], parts, sizes["pc"] // parts), ALL)
    spec = P("pr", ("ph", "pl"), None)
    return jax.shard_map(
        on_device,
        mesh=split,
        in_specs=(spec, P(), P(), P(), P(), P(), P(), P()),
        out_specs=spec,
        check_vma=False,
    )
```

```python
import functools

import jax
import jax.numpy as jnp
from jax import lax
from jax.experimental import pallas as pl
from jax.experimental.pallas import tpu as pltpu
from jax.sharding import Mesh, PartitionSpec as P

F32, BF16 = jnp.float32, jnp.bfloat16
LANES = 128
HALF = ("pr", "pl")
ALL = ("pr", "ph", "pl")
VMEM = pl.BlockSpec(memory_space=pltpu.VMEM)
HBM = pl.BlockSpec(memory_space=pltpu.HBM)


def dot(a, b, over_a, over_b):
    return lax.dot_general(a, b, (((over_a,), (over_b,)), ((), ())), preferred_element_type=F32)


def logistic(v):
    return 0.5 * jnp.tanh(0.5 * v) + 0.5


def params(limit=48 << 20):
    return pltpu.CompilerParams(vmem_limit_bytes=limit)


def cost(flops, nbytes):
    return pl.CostEstimate(flops=flops, bytes_accessed=nbytes, transcendentals=0)


def turned(*refs):
    return jnp.concatenate([r[...].astype(F32).T.astype(BF16) for r in refs], axis=0)


def factor_into(held_ref, rows, weights, take):
    width = weights.shape[0] // 2
    stride = held_ref.shape[0] // width

    def chunk(s, _):
        y = dot(weights, jnp.concatenate([take(2 * s), take(2 * s + 1)], axis=0), 1, 1)
        line = y[:width] * logistic(y[width:])
        for h in range(2):
            held_ref[pl.ds(2 * s + h, width, stride=stride), :] = line[:, h * LANES : (h + 1) * LANES]
        return 0

    lax.fori_loop(0, rows // 2, chunk, 0, unroll=2)
    return held_ref[...].reshape(width, stride, LANES)[:, :rows].astype(BF16)


def left_kernel(x_hbm, w_hbm, g_hbm, out_ref, held_ref, wide_ref, x_ref, w_ref, g_ref, sems):
    copies = [
        pltpu.make_async_copy(a, b, sems.at[i])
        for i, (a, b) in enumerate(((w_hbm, w_ref), (g_hbm, g_ref), (x_hbm, x_ref)))
    ]
    for copy in copies:
        copy.start()
    for copy in copies[:2]:
        copy.wait()
    weights = turned(w_ref, g_ref)
    copies[2].wait()
    lines, ours = x_ref.shape[:2]
    step = ours + 8
    for k in range(lines):
        wide_ref[k * step : k * step + ours, :] = x_ref[k].astype(F32)
    parts = LANES // lines
    rows = ours // parts
    me = lax.axis_index("pr")
    first = [lax.rem(me + parts * t - t, parts) * rows for t in range(parts)]

    def take(s):
        return jnp.concatenate(
            [wide_ref[pl.ds(at + s, lines, stride=step), :] for at in first], axis=0
        ).astype(BF16)

    held = factor_into(held_ref, rows, weights, take)
    pr, ph, pc, size = out_ref.shape[:4]
    held = held.reshape(pr, pc, size, LANES)
    for h in range(ph):
        out_ref[:, h] = held


def right_kernel(fold, x_ref, w_ref, g_ref, *rest):
    outs, held_ref = rest[:-1], rest[-1]
    rows = x_ref.shape[0] // fold

    def take(s):
        parts = [x_ref[e * rows + s] for e in range(fold)]
        return parts[0] if fold == 1 else jnp.concatenate(parts, axis=0)

    held = factor_into(held_ref, rows, turned(w_ref, g_ref), take)
    if len(outs) == 1:
        outs[0][...] = held.reshape(outs[0].shape)
    else:
        me = lax.axis_index(HALF)
        size = outs[0].shape[0]
        per = size // rows
        stride = held_ref.shape[0] // (per * len(outs))
        for s, out in enumerate(outs):
            at = pl.multiple_of((me ^ s) * (per * stride), per * stride)
            block = held_ref[pl.ds(at, per * stride), :].reshape(per, stride, LANES)
            out[...] = block[:, :rows].reshape(size, LANES).astype(BF16)


def gate_kernel(x_ref, og_ref, gain_ref, after_ref, gate_ref, gains_ref):
    lines, ours, depth = x_ref.shape

    def gate(k, _):
        x = x_ref[pl.ds(k * 2, 2)].reshape(2 * ours, depth)
        gate_ref[pl.ds(k * 2, 2)] = logistic(dot(x, og_ref[...], 1, 0)).reshape(2, ours, depth)
        return 0

    lax.fori_loop(0, lines // 2, gate, 0, unroll=2)
    gains_ref[...] = jnp.broadcast_to(gain_ref[...], (LANES, gain_ref.shape[1])).T


def slots(shape, count):
    return lax.broadcasted_iota(jnp.int32, shape, 1) // (LANES // count)


def pick(values):
    out = values[0]
    for t, value in enumerate(values[1:], 1):
        out = jnp.where(slots(out.shape, len(values)) == t, value, out)
    return out


def roll(value, by):
    by = by % LANES
    return value if by == 0 else pltpu.roll(value, by, 1)


def left_of(ref, ch, lines):
    pr, pc = ref.shape[:2]
    parts = LANES // lines
    bands = []
    for q in range(parts):
        tiles = []
        for g in range(0, pr, parts):
            cols = [
                roll(pick([ref[g + (t + q) % parts, c, ch] for t in range(parts)]), lines * q)
                for c in range(pc)
            ]
            tiles.append(jnp.concatenate(cols, axis=0))
        bands.append(jnp.concatenate(tiles, axis=1))
    return jnp.concatenate(bands, axis=0)


def right_of(get, pr, pc, fold):
    width = LANES // fold
    bands = []
    for p in range(pr):
        turns = [[roll(get(p, c), width * t) for t in range(fold)] for c in range(pc)]
        for e in range(fold):
            tiles = [pick([turn[(t - e) % fold] for t in range(fold)]) for turn in turns]
            bands.append(jnp.concatenate(tiles, axis=1))
    return jnp.concatenate(bands, axis=0)


def product_kernel(fold, scale, left_ref, after_ref, *rest):
    rights, out_ref, held = rest[:-2], *rest[-2:]
    rows_of, pc, channels, rows = out_ref.shape[:4]
    pr, blocks = left_ref.shape[:2]
    if len(rights) > 1:
        me = lax.axis_index(HALF)
        for s, right in enumerate(rights):
            held[me ^ s] = right[...]

    for ch in range(channels):
        left = left_of(left_ref, ch, rows * fold)
        if len(rights) > 1:
            at = slice(ch * rows, (ch + 1) * rows)
            right = right_of(lambda p, c: held[p * pc + c, at, :], pr, pc, fold)
        else:
            right = right_of(lambda p, c: rights[0][p, c, ch], pr, pc, fold)
        mixed = dot(left, right, 1, 0) * scale
        for p in range(rows_of):
            block, part = divmod(p, rows_of // blocks)
            at = [((part * fold + f) * blocks + block) * rows for f in range(fold)]
            for c in range(pc):
                lanes = slice(c * LANES, (c + 1) * LANES)
                out_ref[p, c, ch] = pick([mixed[a : a + rows, lanes] for a in at]).astype(BF16)


def pair_kernel(fold, mixed_ref, gate_ref, gains_ref, ow_ref, out_ref, held_ref):
    depth, rows = mixed_ref.shape[:2]
    stride = held_ref.shape[1]
    width = LANES // fold
    held_ref[:, :rows] = mixed_ref[...].astype(F32)
    flat_ref = held_ref.reshape(depth * stride, LANES)
    gain, weight = gains_ref[...], ow_ref[...]
    for s in range(rows):
        v = flat_ref[pl.ds(s, depth, stride=stride), :]
        centred = v - jnp.sum(v, axis=0, keepdims=True) * (1.0 / depth)
        spread = jnp.sum(centred * centred, axis=0, keepdims=True) * (1.0 / depth)
        scaled = (centred * lax.rsqrt(spread + 1e-05) * gain).astype(BF16)
        y = dot(scaled, weight, 0, 0)
        for f in range(fold):
            at = f * rows + s
            out_ref[at] = (y[f * width : (f + 1) * width] * gate_ref[at]).astype(BF16)


def on_device(
    pair_array, left_weight, right_weight, left_gate, right_gate, mid_gain, out_weight, out_gate
):
    pr, ph, pc = lax.axis_size("pr"), lax.axis_size("ph"), lax.axis_size("pl")
    m = pr * pc
    lines, ours, depth = pair_array.shape
    mix = left_weight.shape[1]
    count = lines * pr
    fold = max(1, LANES // ours)
    rows = lines * ours // LANES
    channels = mix // m
    size = channels * rows
    hops = m <= 16 and m & (m - 1) == 0
    n_x = pair_array.size
    flops = 4 * lines * ours * depth * mix
    held = pltpu.VMEM((mix * (rows + 8), LANES), F32)

    left = pl.pallas_call(
        left_kernel,
        out_shape=jax.ShapeDtypeStruct((pr, ph, pc, size, LANES), BF16),
        in_specs=[HBM] * 3,
        out_specs=VMEM,
        scratch_shapes=[
            held,
            pltpu.VMEM((lines * (ours + 8), depth), F32),
            *[pltpu.VMEM(a.shape, BF16) for a in (pair_array, left_weight, left_gate)],
            pltpu.SemaphoreType.DMA((3,)),
        ],
        compiler_params=params(67043328),
        cost_estimate=cost(flops, 4 * n_x),
        name="left",
    )(pair_array, left_weight, left_gate)
    left = lax.all_to_all(left.reshape(pr * ph * pc, size, LANES), ALL, 0, 0, tiled=True)
    left = left.reshape(pr, ph * pc, channels, rows, LANES)

    if hops:
        shapes = [jax.ShapeDtypeStruct((size, LANES), BF16)] * m
    else:
        shapes = [jax.ShapeDtypeStruct((m, size, LANES), BF16)]
    right = pl.pallas_call(
        functools.partial(right_kernel, fold),
        out_shape=shapes,
        in_specs=[VMEM] * 3,
        out_specs=[VMEM] * len(shapes),
        scratch_shapes=[held],
        compiler_params=params(),
        cost_estimate=cost(flops, 4 * n_x),
        name="right",
    )(pair_array, right_weight, right_gate)
    gate, gains = pl.pallas_call(
        gate_kernel,
        out_shape=[
            jax.ShapeDtypeStruct(pair_array.shape, F32),
            jax.ShapeDtypeStruct((mix, LANES), F32),
        ],
        in_specs=[VMEM] * 4,
        out_specs=[VMEM] * 2,
        compiler_params=params(),
        cost_estimate=cost(flops // 2, 4 * n_x),
        name="gate",
    )(pair_array, out_gate, mid_gain.reshape(1, mix), right[0])
    if hops:
        right = list(right)
        for s in sorted(range(1, m), key=lambda s: s % pc == 0):
            right[s] = lax.ppermute(right[s], HALF, [(i, i ^ s) for i in range(m)])
    else:
        right = [lax.all_to_all(right[0], HALF, 0, 0, tiled=True)]
        right = [right[0].reshape(pr, pc, channels, rows, LANES)]

    if hops:
        at_once, blocks = channels, ph * pc
        right_specs = [pl.BlockSpec((size, LANES), lambda h, c: (0, 0))] * m
        kept = pltpu.VMEM((m, size, LANES), BF16)
    else:
        at_once, blocks = 1, 1
        right_specs = [
            pl.BlockSpec((pr, pc, at_once, rows, LANES), lambda h, c: (0, 0, h, 0, 0))
        ]
        kept = pltpu.VMEM((8, LANES), BF16)
    mixed = pl.pallas_call(
        functools.partial(product_kernel, fold, count ** (-0.5)),
        grid=(channels // at_once, ph * pc // blocks),
        out_shape=jax.ShapeDtypeStruct((pr, pc, channels, rows, LANES), BF16),
        in_specs=[
            pl.BlockSpec((pr, blocks, at_once, rows, LANES), lambda h, c: (0, c, h, 0, 0)),
            pl.BlockSpec((8, LANES), lambda h, c: (0, 0)),
            *right_specs,
        ],
        out_specs=pl.BlockSpec(
            (pr * blocks // (ph * pc), pc, at_once, rows, LANES), lambda h, c: (c, 0, h, 0, 0)
        ),
        scratch_shapes=[kept],
        compiler_params=params(),
        cost_estimate=cost(2 * count * count * ours * pc * channels, 8 * n_x),
        name="product",
    )(left, gains, *right)
    mixed = lax.all_to_all(mixed.reshape(m, size, LANES), HALF, 0, 0, tiled=True)
    return pl.pallas_call(
        functools.partial(pair_kernel, fold),
        out_shape=jax.ShapeDtypeStruct(pair_array.shape, BF16),
        in_specs=[VMEM] * 4,
        out_specs=VMEM,
        scratch_shapes=[pltpu.VMEM((mix, rows + 8, LANES), F32)],
        compiler_params=params(),
        cost_estimate=cost(flops // 2, 8 * n_x),
        name="pair",
    )(mixed.reshape(mix, rows, LANES), gate, gains, out_weight)


def solution(mesh):
    sizes = dict(mesh.shape)
    parts = 2 if sizes["pc"] % 2 == 0 else 1
    split = Mesh(mesh.devices.reshape(sizes["pr"], parts, sizes["pc"] // parts), ALL)
    spec = P("pr", ("ph", "pl"), None)
    return jax.shard_map(
        on_device,
        mesh=split,
        in_specs=(spec, P(), P(), P(), P(), P(), P(), P()),
        out_specs=spec,
        check_vma=False,
    )
```

```python
import functools

import jax
import jax.numpy as jnp
from jax import lax
from jax.experimental import pallas as pl
from jax.experimental.pallas import tpu as pltpu
from jax.sharding import Mesh, PartitionSpec as P

F32, BF16 = jnp.float32, jnp.bfloat16
LANES = 128
HALF = ("pr", "pl")
ALL = ("pr", "ph", "pl")
VMEM = pl.BlockSpec(memory_space=pltpu.VMEM)
HBM = pl.BlockSpec(memory_space=pltpu.HBM)


def dot(a, b, over_a, over_b):
    return lax.dot_general(a, b, (((over_a,), (over_b,)), ((), ())), preferred_element_type=F32)


def logistic(v):
    return 0.5 * jnp.tanh(0.5 * v) + 0.5


def params(limit=48 << 20):
    return pltpu.CompilerParams(vmem_limit_bytes=limit)


def cost(flops, nbytes):
    return pl.CostEstimate(flops=flops, bytes_accessed=nbytes, transcendentals=0)


def turned(*refs):
    return jnp.concatenate([r[...].astype(F32).T.astype(BF16) for r in refs], axis=0)


def factor_into(held_ref, rows, weights, take):
    width = weights.shape[0] // 2
    stride = held_ref.shape[0] // width

    def chunk(s, _):
        y = dot(weights, jnp.concatenate([take(2 * s), take(2 * s + 1)], axis=0), 1, 1)
        line = y[:width] * logistic(y[width:])
        for h in range(2):
            held_ref[pl.ds(2 * s + h, width, stride=stride), :] = line[:, h * LANES : (h + 1) * LANES]
        return 0

    lax.fori_loop(0, rows // 2, chunk, 0, unroll=8)


def lines_in(held_ref, first, count, rows, stride):
    held = held_ref[pl.ds(first * stride, count * stride), :].reshape(count, stride, LANES)
    return held[:, :rows].reshape(count * rows, LANES).astype(BF16)


def left_kernel(
    x_hbm, w_hbm, g_hbm, out_hbm, held_ref, wide_ref, x_ref, w_ref, g_ref, out_ref, sems, out_sems
):
    copies = [
        pltpu.make_async_copy(a, b, sems.at[i])
        for i, (a, b) in enumerate(((w_hbm, w_ref), (g_hbm, g_ref), (x_hbm, x_ref)))
    ]
    for copy in copies:
        copy.start()
    for copy in copies[:2]:
        copy.wait()
    weights = turned(w_ref, g_ref)
    copies[2].wait()
    lines, ours = x_ref.shape[:2]
    step = ours + 8
    for k in range(lines):
        wide_ref[k * step : k * step + ours, :] = x_ref[k].astype(F32)
    parts = LANES // lines
    rows = ours // parts
    me = lax.axis_index("pr")
    first = [lax.rem(me + parts * t - t, parts) * rows for t in range(parts)]

    def take(s):
        return jnp.concatenate(
            [wide_ref[pl.ds(at + s, lines, stride=step), :] for at in first], axis=0
        ).astype(BF16)

    factor_into(held_ref, rows, weights, take)
    groups, ph = out_sems.shape
    pr, pc, size = out_ref.shape[:3]
    span = pr // groups
    count = span * pc * size // rows
    copies = []
    for g in range(groups):
        part = pl.ds(g * span, span)
        lines = lines_in(held_ref, g * count, count, rows, rows + 8)
        out_ref[part] = lines.reshape(span, pc, size, LANES)
        for h in range(ph):
            copy = pltpu.make_async_copy(out_ref.at[part], out_hbm.at[part, h], out_sems.at[g, h])
            copy.start()
            copies.append(copy)
    for copy in copies:
        copy.wait()


def right_kernel(fold, x_ref, w_ref, g_ref, *rest):
    outs, held_ref = rest[:-1], rest[-1]
    rows = x_ref.shape[0] // fold

    def take(s):
        parts = [x_ref[e * rows + s] for e in range(fold)]
        return parts[0] if fold == 1 else jnp.concatenate(parts, axis=0)

    factor_into(held_ref, rows, turned(w_ref, g_ref), take)
    stride = rows + 8
    if len(outs) == 1:
        count = held_ref.shape[0] // stride
        outs[0][...] = lines_in(held_ref, 0, count, rows, stride).reshape(outs[0].shape)
    else:
        me = lax.axis_index(HALF)
        count = outs[0].shape[0] // rows
        for s, out in enumerate(outs):
            out[...] = lines_in(held_ref, (me ^ s) * count, count, rows, stride)


def gate_kernel(x_ref, og_ref, gain_ref, after_ref, gate_ref, gains_ref):
    lines, ours, depth = x_ref.shape

    def gate(k, _):
        x = x_ref[pl.ds(k * 2, 2)].reshape(2 * ours, depth)
        gate_ref[pl.ds(k * 2, 2)] = logistic(dot(x, og_ref[...], 1, 0)).reshape(2, ours, depth)
        return 0

    lax.fori_loop(0, lines // 2, gate, 0, unroll=2)
    gains_ref[...] = jnp.broadcast_to(gain_ref[...], (LANES, gain_ref.shape[1])).T


def slots(shape, count):
    return lax.broadcasted_iota(jnp.int32, shape, 1) // (LANES // count)


def pick(values):
    out = values[0]
    for t, value in enumerate(values[1:], 1):
        out = jnp.where(slots(out.shape, len(values)) == t, value, out)
    return out


def roll(value, by):
    by = by % LANES
    return value if by == 0 else pltpu.roll(value, by, 1)


def left_of(ref, ch, lines):
    pr, pc = ref.shape[:2]
    parts = LANES // lines
    bands = []
    for q in range(parts):
        tiles = []
        for g in range(0, pr, parts):
            cols = [
                roll(pick([ref[g + (t + q) % parts, c, ch] for t in range(parts)]), lines * q)
                for c in range(pc)
            ]
            tiles.append(jnp.concatenate(cols, axis=0))
        bands.append(jnp.concatenate(tiles, axis=1))
    return jnp.concatenate(bands, axis=0)


def right_of(get, pr, pc, fold):
    width = LANES // fold
    bands = []
    for p in range(pr):
        turns = [[roll(get(p, c), width * t) for t in range(fold)] for c in range(pc)]
        for e in range(fold):
            tiles = [pick([turn[(t - e) % fold] for t in range(fold)]) for turn in turns]
            bands.append(jnp.concatenate(tiles, axis=1))
    return jnp.concatenate(bands, axis=0)


def product_kernel(fold, scale, left_ref, after_ref, *rest):
    rights, out_ref, held = rest[:-2], *rest[-2:]
    rows_of, pc, channels, rows = out_ref.shape[:4]
    pr, blocks = left_ref.shape[:2]
    if len(rights) > 1:
        me = lax.axis_index(HALF)
        for s, right in enumerate(rights):
            held[me ^ s] = right[...]

    for ch in range(channels):
        left = left_of(left_ref, ch, rows * fold)
        if len(rights) > 1:
            at = slice(ch * rows, (ch + 1) * rows)
            right = right_of(lambda p, c: held[p * pc + c, at, :], pr, pc, fold)
        else:
            right = right_of(lambda p, c: rights[0][p, c, ch], pr, pc, fold)
        mixed = dot(left, right, 1, 0) * scale
        for p in range(rows_of):
            block, part = divmod(p, rows_of // blocks)
            at = [((part * fold + f) * blocks + block) * rows for f in range(fold)]
            for c in range(pc):
                lanes = slice(c * LANES, (c + 1) * LANES)
                out_ref[p, c, ch] = pick([mixed[a : a + rows, lanes] for a in at]).astype(BF16)


def pair_kernel(fold, mixed_ref, gate_ref, gains_ref, ow_ref, out_hbm, held_ref, out_ref, sems):
    depth, rows = mixed_ref.shape[:2]
    stride = held_ref.shape[1]
    width = LANES // fold
    held_ref[:, :rows] = mixed_ref[...].astype(F32)
    flat_ref = held_ref.reshape(depth * stride, LANES)
    gain, weight = gains_ref[...], ow_ref[...]
    span = rows // sems.shape[0]
    copies = []
    for s in range(rows):
        v = flat_ref[pl.ds(s, depth, stride=stride), :]
        centred = v - jnp.sum(v, axis=0, keepdims=True) * (1.0 / depth)
        spread = jnp.sum(centred * centred, axis=0, keepdims=True) * (1.0 / depth)
        scaled = (centred * lax.rsqrt(spread + 1e-05) * gain).astype(BF16)
        y = dot(scaled, weight, 0, 0)
        for f in range(fold):
            at = f * rows + s
            out_ref[at] = (y[f * width : (f + 1) * width] * gate_ref[at]).astype(BF16)
        if (s + 1) % span == 0:
            for f in range(fold):
                part = pl.ds(f * rows + s + 1 - span, span)
                copy = pltpu.make_async_copy(
                    out_ref.at[part], out_hbm.at[part], sems.at[s // span, f]
                )
                copy.start()
                copies.append(copy)
    for copy in copies:
        copy.wait()


def on_device(
    pair_array, left_weight, right_weight, left_gate, right_gate, mid_gain, out_weight, out_gate
):
    pr, ph, pc = lax.axis_size("pr"), lax.axis_size("ph"), lax.axis_size("pl")
    m = pr * pc
    lines, ours, depth = pair_array.shape
    mix = left_weight.shape[1]
    count = lines * pr
    fold = max(1, LANES // ours)
    rows = lines * ours // LANES
    channels = mix // m
    size = channels * rows
    hops = m <= 16 and m & (m - 1) == 0
    n_x = pair_array.size
    flops = 4 * lines * ours * depth * mix
    held = pltpu.VMEM((mix * (rows + 8), LANES), F32)

    left = pl.pallas_call(
        left_kernel,
        out_shape=jax.ShapeDtypeStruct((pr, ph, pc, size, LANES), BF16),
        in_specs=[HBM] * 3,
        out_specs=HBM,
        scratch_shapes=[
            held,
            pltpu.VMEM((lines * (ours + 8), depth), F32),
            *[pltpu.VMEM(a.shape, BF16) for a in (pair_array, left_weight, left_gate)],
            pltpu.VMEM((pr, pc, size, LANES), BF16),
            pltpu.SemaphoreType.DMA((3,)),
            pltpu.SemaphoreType.DMA((4, ph)),
        ],
        compiler_params=params(67043328),
        cost_estimate=cost(flops, 4 * n_x),
        name="left",
    )(pair_array, left_weight, left_gate)
    left = lax.all_to_all(left.reshape(pr * ph * pc, size, LANES), ALL, 0, 0, tiled=True)
    left = left.reshape(pr, ph * pc, channels, rows, LANES)

    if hops:
        shapes = [jax.ShapeDtypeStruct((size, LANES), BF16)] * m
    else:
        shapes = [jax.ShapeDtypeStruct((m, size, LANES), BF16)]
    right = pl.pallas_call(
        functools.partial(right_kernel, fold),
        out_shape=shapes,
        in_specs=[VMEM] * 3,
        out_specs=[VMEM] * len(shapes),
        scratch_shapes=[held],
        compiler_params=params(),
        cost_estimate=cost(flops, 4 * n_x),
        name="right",
    )(pair_array, right_weight, right_gate)
    gate, gains = pl.pallas_call(
        gate_kernel,
        out_shape=[
            jax.ShapeDtypeStruct(pair_array.shape, F32),
            jax.ShapeDtypeStruct((mix, LANES), F32),
        ],
        in_specs=[VMEM] * 4,
        out_specs=[VMEM] * 2,
        compiler_params=params(),
        cost_estimate=cost(flops // 2, 4 * n_x),
        name="gate",
    )(pair_array, out_gate, mid_gain.reshape(1, mix), right[0])
    if hops:
        right = list(right)
        for s in sorted(range(1, m), key=lambda s: s % pc == 0):
            right[s] = lax.ppermute(right[s], HALF, [(i, i ^ s) for i in range(m)])
    else:
        right = [lax.all_to_all(right[0], HALF, 0, 0, tiled=True)]
        right = [right[0].reshape(pr, pc, channels, rows, LANES)]

    if hops:
        at_once, blocks = channels, ph * pc
        right_specs = [pl.BlockSpec((size, LANES), lambda h, c: (0, 0))] * m
        kept = pltpu.VMEM((m, size, LANES), BF16)
    else:
        at_once, blocks = 1, 1
        right_specs = [
            pl.BlockSpec((pr, pc, at_once, rows, LANES), lambda h, c: (0, 0, h, 0, 0))
        ]
        kept = pltpu.VMEM((8, LANES), BF16)
    mixed = pl.pallas_call(
        functools.partial(product_kernel, fold, count ** (-0.5)),
        grid=(channels // at_once, ph * pc // blocks),
        out_shape=jax.ShapeDtypeStruct((pr, pc, channels, rows, LANES), BF16),
        in_specs=[
            pl.BlockSpec((pr, blocks, at_once, rows, LANES), lambda h, c: (0, c, h, 0, 0)),
            pl.BlockSpec((8, LANES), lambda h, c: (0, 0)),
            *right_specs,
        ],
        out_specs=pl.BlockSpec(
            (pr * blocks // (ph * pc), pc, at_once, rows, LANES), lambda h, c: (c, 0, h, 0, 0)
        ),
        scratch_shapes=[kept],
        compiler_params=params(),
        cost_estimate=cost(2 * count * count * ours * pc * channels, 8 * n_x),
        name="product",
    )(left, gains, *right)
    mixed = lax.all_to_all(mixed.reshape(m, size, LANES), HALF, 0, 0, tiled=True)
    return pl.pallas_call(
        functools.partial(pair_kernel, fold),
        out_shape=jax.ShapeDtypeStruct(pair_array.shape, BF16),
        in_specs=[VMEM] * 4,
        out_specs=HBM,
        scratch_shapes=[
            pltpu.VMEM((mix, rows + 8, LANES), F32),
            pltpu.VMEM(pair_array.shape, BF16),
            pltpu.SemaphoreType.DMA((4, fold)),
        ],
        compiler_params=params(),
        cost_estimate=cost(flops // 2, 8 * n_x),
        name="pair",
    )(mixed.reshape(mix, rows, LANES), gate, gains, out_weight)


def solution(mesh):
    sizes = dict(mesh.shape)
    parts = 2 if sizes["pc"] % 2 == 0 else 1
    split = Mesh(mesh.devices.reshape(sizes["pr"], parts, sizes["pc"] // parts), ALL)
    spec = P("pr", ("ph", "pl"), None)
    return jax.shard_map(
        on_device,
        mesh=split,
        in_specs=(spec, P(), P(), P(), P(), P(), P(), P()),
        out_specs=spec,
        check_vma=False,
    )
```

```python
import functools

import jax
import jax.numpy as jnp
from jax import lax
from jax.experimental import pallas as pl
from jax.experimental.pallas import tpu as pltpu
from jax.sharding import Mesh, PartitionSpec as P

F32, BF16 = jnp.float32, jnp.bfloat16
LANES = 128
HALF = ("pr", "pl")
ALL = ("pr", "ph", "pl")
VMEM = pl.BlockSpec(memory_space=pltpu.VMEM)
HBM = pl.BlockSpec(memory_space=pltpu.HBM)


def dot(a, b, over_a, over_b):
    return lax.dot_general(a, b, (((over_a,), (over_b,)), ((), ())), preferred_element_type=F32)


def logistic(v):
    return 0.5 * jnp.tanh(0.5 * v) + 0.5


def params(limit=48 << 20):
    return pltpu.CompilerParams(vmem_limit_bytes=limit)


def cost(flops, nbytes):
    return pl.CostEstimate(flops=flops, bytes_accessed=nbytes, transcendentals=0)


def turned(*refs):
    return jnp.concatenate([r[...].astype(F32).T.astype(BF16) for r in refs], axis=0)


def factor_into(held_ref, rows, weights, take):
    width = weights.shape[0] // 2
    stride = held_ref.shape[0] // width

    def chunk(s, _):
        y = dot(weights, jnp.concatenate([take(2 * s), take(2 * s + 1)], axis=0), 1, 1)
        line = y[:width] * logistic(y[width:])
        for h in range(2):
            held_ref[pl.ds(2 * s + h, width, stride=stride), :] = line[:, h * LANES : (h + 1) * LANES]
        return 0

    lax.fori_loop(0, rows // 2, chunk, 0, unroll=8)


def lines_in(held_ref, first, count, rows, stride):
    held = held_ref[pl.ds(first * stride, count * stride), :].reshape(count, stride, LANES)
    return held[:, :rows].reshape(count * rows, LANES).astype(BF16)


def left_kernel(
    x_hbm, w_hbm, g_hbm, out_hbm, held_ref, wide_ref, x_ref, w_ref, g_ref, out_ref, sems, out_sems
):
    lines, ours = x_ref.shape[:2]
    pieces, step = sems.shape[0] - 2, ours + 8
    whole = [(w_hbm, w_ref), (g_hbm, g_ref)]
    for i in range(pieces):
        part = pl.ds(i * lines // pieces, lines // pieces)
        whole.append((x_hbm.at[part], x_ref.at[part]))
    copies = [pltpu.make_async_copy(a, b, sems.at[i]) for i, (a, b) in enumerate(whole)]
    for copy in copies[2:] + copies[:2]:
        copy.start()
    for i in range(pieces):
        copies[2 + i].wait()
        for k in range(i * lines // pieces, (i + 1) * lines // pieces):
            wide_ref[k * step : k * step + ours, :] = x_ref[k].astype(F32)
    parts = LANES // lines
    rows = ours // parts
    me = lax.axis_index("pr")
    first = [lax.rem(me + parts * t - t, parts) * rows for t in range(parts)]
    for copy in copies[:2]:
        copy.wait()
    weights = turned(w_ref), turned(g_ref)
    taken = [
        jnp.concatenate(
            [wide_ref[pl.ds(at + s, lines, stride=step), :] for at in first], axis=0
        ).astype(BF16)
        for s in range(rows)
    ]
    groups, ph = out_sems.shape
    pr, pc, size = out_ref.shape[:3]
    span = pr // groups
    count, stride = span * pc * size // rows, rows + 8
    copies = []
    for g in range(groups):
        mine = jnp.concatenate([w[g * count : (g + 1) * count] for w in weights], axis=0)
        for s in range(0, rows, 2):
            y = dot(mine, jnp.concatenate(taken[s : s + 2], axis=0), 1, 1)
            line = y[:count] * logistic(y[count:])
            for h in range(2):
                at = pl.ds(g * count * stride + s + h, count, stride=stride)
                held_ref[at, :] = line[:, h * LANES : (h + 1) * LANES]
        part = pl.ds(g * span, span)
        held = lines_in(held_ref, g * count, count, rows, stride)
        out_ref[part] = held.reshape(span, pc, size, LANES)
        for h in range(ph):
            copy = pltpu.make_async_copy(out_ref.at[part], out_hbm.at[part, h], out_sems.at[g, h])
            copy.start()
            copies.append(copy)
    for copy in copies:
        copy.wait()


def right_kernel(fold, x_ref, w_ref, g_ref, *rest):
    outs, held_ref = rest[:-1], rest[-1]
    rows = x_ref.shape[0] // fold

    def take(s):
        parts = [x_ref[e * rows + s] for e in range(fold)]
        return parts[0] if fold == 1 else jnp.concatenate(parts, axis=0)

    factor_into(held_ref, rows, turned(w_ref, g_ref), take)
    stride = rows + 8
    if len(outs) == 1:
        count = held_ref.shape[0] // stride
        outs[0][...] = lines_in(held_ref, 0, count, rows, stride).reshape(outs[0].shape)
    else:
        me = lax.axis_index(HALF)
        count = outs[0].shape[0] // rows
        for s, out in enumerate(outs):
            out[...] = lines_in(held_ref, (me ^ s) * count, count, rows, stride)


def gate_kernel(x_ref, og_ref, gain_ref, after_ref, gate_ref, gains_ref):
    lines, ours, depth = x_ref.shape

    def gate(k, _):
        x = x_ref[pl.ds(k * 2, 2)].reshape(2 * ours, depth)
        gate_ref[pl.ds(k * 2, 2)] = logistic(dot(x, og_ref[...], 1, 0)).reshape(2, ours, depth)
        return 0

    lax.fori_loop(0, lines // 2, gate, 0, unroll=2)
    gains_ref[...] = jnp.broadcast_to(gain_ref[...], (LANES, gain_ref.shape[1])).T


def slots(shape, count):
    return lax.broadcasted_iota(jnp.int32, shape, 1) // (LANES // count)


def pick(values):
    out = values[0]
    for t, value in enumerate(values[1:], 1):
        out = jnp.where(slots(out.shape, len(values)) == t, value, out)
    return out


def roll(value, by):
    by = by % LANES
    return value if by == 0 else pltpu.roll(value, by, 1)


def left_of(ref, ch, lines):
    pr, pc = ref.shape[:2]
    parts = LANES // lines
    bands = []
    for q in range(parts):
        tiles = []
        for g in range(0, pr, parts):
            cols = [
                roll(pick([ref[g + (t + q) % parts, c, ch] for t in range(parts)]), lines * q)
                for c in range(pc)
            ]
            tiles.append(jnp.concatenate(cols, axis=0))
        bands.append(jnp.concatenate(tiles, axis=1))
    return jnp.concatenate(bands, axis=0)


def right_of(get, pr, pc, fold):
    width = LANES // fold
    bands = []
    for p in range(pr):
        turns = [[roll(get(p, c), width * t) for t in range(fold)] for c in range(pc)]
        for e in range(fold):
            tiles = [pick([turn[(t - e) % fold] for t in range(fold)]) for turn in turns]
            bands.append(jnp.concatenate(tiles, axis=1))
    return jnp.concatenate(bands, axis=0)


def product_kernel(fold, scale, left_ref, after_ref, *rest):
    rights, out_ref, held = rest[:-2], *rest[-2:]
    rows_of, pc, channels, rows = out_ref.shape[:4]
    pr, blocks = left_ref.shape[:2]
    if len(rights) > 1:
        me = lax.axis_index(HALF)
        for s, right in enumerate(rights):
            held[me ^ s] = right[...]

    for ch in range(channels):
        left = left_of(left_ref, ch, rows * fold)
        if len(rights) > 1:
            at = slice(ch * rows, (ch + 1) * rows)
            right = right_of(lambda p, c: held[p * pc + c, at, :], pr, pc, fold)
        else:
            right = right_of(lambda p, c: rights[0][p, c, ch], pr, pc, fold)
        mixed = dot(left, right, 1, 0) * scale
        for p in range(rows_of):
            block, part = divmod(p, rows_of // blocks)
            at = [((part * fold + f) * blocks + block) * rows for f in range(fold)]
            for c in range(pc):
                lanes = slice(c * LANES, (c + 1) * LANES)
                out_ref[p, c, ch] = pick([mixed[a : a + rows, lanes] for a in at]).astype(BF16)


def pair_kernel(fold, mixed_ref, gate_ref, gains_ref, ow_ref, out_hbm, held_ref, out_ref, sems):
    depth, rows = mixed_ref.shape[:2]
    stride = held_ref.shape[1]
    width = LANES // fold
    held_ref[:, :rows] = mixed_ref[...].astype(F32)
    flat_ref = held_ref.reshape(depth * stride, LANES)
    gain, weight = gains_ref[...], ow_ref[...]
    span = rows // sems.shape[0]
    copies = []
    for s in range(rows):
        v = flat_ref[pl.ds(s, depth, stride=stride), :]
        centred = v - jnp.sum(v, axis=0, keepdims=True) * (1.0 / depth)
        spread = jnp.sum(centred * centred, axis=0, keepdims=True) * (1.0 / depth)
        scaled = (centred * lax.rsqrt(spread + 1e-05) * gain).astype(BF16)
        y = dot(scaled, weight, 0, 0)
        for f in range(fold):
            at = f * rows + s
            out_ref[at] = (y[f * width : (f + 1) * width] * gate_ref[at]).astype(BF16)
        if (s + 1) % span == 0:
            for f in range(fold):
                part = pl.ds(f * rows + s + 1 - span, span)
                copy = pltpu.make_async_copy(
                    out_ref.at[part], out_hbm.at[part], sems.at[s // span, f]
                )
                copy.start()
                copies.append(copy)
    for copy in copies:
        copy.wait()


def on_device(
    pair_array, left_weight, right_weight, left_gate, right_gate, mid_gain, out_weight, out_gate
):
    pr, ph, pc = lax.axis_size("pr"), lax.axis_size("ph"), lax.axis_size("pl")
    m = pr * pc
    lines, ours, depth = pair_array.shape
    mix = left_weight.shape[1]
    count = lines * pr
    fold = max(1, LANES // ours)
    rows = lines * ours // LANES
    channels = mix // m
    size = channels * rows
    hops = m <= 16 and m & (m - 1) == 0
    n_x = pair_array.size
    flops = 4 * lines * ours * depth * mix
    held = pltpu.VMEM((mix * (rows + 8), LANES), F32)

    left = pl.pallas_call(
        left_kernel,
        out_shape=jax.ShapeDtypeStruct((pr, ph, pc, size, LANES), BF16),
        in_specs=[HBM] * 3,
        out_specs=HBM,
        scratch_shapes=[
            held,
            pltpu.VMEM((lines * (ours + 8), depth), F32),
            *[pltpu.VMEM(a.shape, BF16) for a in (pair_array, left_weight, left_gate)],
            pltpu.VMEM((pr, pc, size, LANES), BF16),
            pltpu.SemaphoreType.DMA((4,)),
            pltpu.SemaphoreType.DMA((2, ph)),
        ],
        compiler_params=params(67043328),
        cost_estimate=cost(flops, 4 * n_x),
        name="left",
    )(pair_array, left_weight, left_gate)
    left = lax.all_to_all(left.reshape(pr * ph * pc, size, LANES), ALL, 0, 0, tiled=True)
    left = left.reshape(pr, ph * pc, channels, rows, LANES)

    if hops:
        shapes = [jax.ShapeDtypeStruct((size, LANES), BF16)] * m
    else:
        shapes = [jax.ShapeDtypeStruct((m, size, LANES), BF16)]
    right = pl.pallas_call(
        functools.partial(right_kernel, fold),
        out_shape=shapes,
        in_specs=[VMEM] * 3,
        out_specs=[VMEM] * len(shapes),
        scratch_shapes=[held],
        compiler_params=params(),
        cost_estimate=cost(flops, 4 * n_x),
        name="right",
    )(pair_array, right_weight, right_gate)
    gate, gains = pl.pallas_call(
        gate_kernel,
        out_shape=[
            jax.ShapeDtypeStruct(pair_array.shape, F32),
            jax.ShapeDtypeStruct((mix, LANES), F32),
        ],
        in_specs=[VMEM] * 4,
        out_specs=[VMEM] * 2,
        compiler_params=params(),
        cost_estimate=cost(flops // 2, 4 * n_x),
        name="gate",
    )(pair_array, out_gate, mid_gain.reshape(1, mix), right[0])
    if hops:
        right = list(right)
        for s in sorted(range(1, m), key=lambda s: s % pc == 0):
            right[s] = lax.ppermute(right[s], HALF, [(i, i ^ s) for i in range(m)])
    else:
        right = [lax.all_to_all(right[0], HALF, 0, 0, tiled=True)]
        right = [right[0].reshape(pr, pc, channels, rows, LANES)]

    if hops:
        at_once, blocks = channels, ph * pc
        right_specs = [pl.BlockSpec((size, LANES), lambda h, c: (0, 0))] * m
        kept = pltpu.VMEM((m, size, LANES), BF16)
    else:
        at_once, blocks = 1, 1
        right_specs = [
            pl.BlockSpec((pr, pc, at_once, rows, LANES), lambda h, c: (0, 0, h, 0, 0))
        ]
        kept = pltpu.VMEM((8, LANES), BF16)
    mixed = pl.pallas_call(
        functools.partial(product_kernel, fold, count ** (-0.5)),
        grid=(channels // at_once, ph * pc // blocks),
        out_shape=jax.ShapeDtypeStruct((pr, pc, channels, rows, LANES), BF16),
        in_specs=[
            pl.BlockSpec((pr, blocks, at_once, rows, LANES), lambda h, c: (0, c, h, 0, 0)),
            pl.BlockSpec((8, LANES), lambda h, c: (0, 0)),
            *right_specs,
        ],
        out_specs=pl.BlockSpec(
            (pr * blocks // (ph * pc), pc, at_once, rows, LANES), lambda h, c: (c, 0, h, 0, 0)
        ),
        scratch_shapes=[kept],
        compiler_params=params(),
        cost_estimate=cost(2 * count * count * ours * pc * channels, 8 * n_x),
        name="product",
    )(left, gains, *right)
    mixed = lax.all_to_all(mixed.reshape(m, size, LANES), HALF, 0, 0, tiled=True)
    return pl.pallas_call(
        functools.partial(pair_kernel, fold),
        out_shape=jax.ShapeDtypeStruct(pair_array.shape, BF16),
        in_specs=[VMEM] * 4,
        out_specs=HBM,
        scratch_shapes=[
            pltpu.VMEM((mix, rows + 8, LANES), F32),
            pltpu.VMEM(pair_array.shape, BF16),
            pltpu.SemaphoreType.DMA((4, fold)),
        ],
        compiler_params=params(),
        cost_estimate=cost(flops // 2, 8 * n_x),
        name="pair",
    )(mixed.reshape(mix, rows, LANES), gate, gains, out_weight)


def solution(mesh):
    sizes = dict(mesh.shape)
    parts = 2 if sizes["pc"] % 2 == 0 else 1
    split = Mesh(mesh.devices.reshape(sizes["pr"], parts, sizes["pc"] // parts), ALL)
    spec = P("pr", ("ph", "pl"), None)
    return jax.shard_map(
        on_device,
        mesh=split,
        in_specs=(spec, P(), P(), P(), P(), P(), P(), P()),
        out_specs=spec,
        check_vma=False,
    )
```

```python
import functools

import jax
import jax.numpy as jnp
from jax import lax
from jax.experimental import pallas as pl
from jax.experimental.pallas import tpu as pltpu
from jax.sharding import Mesh, PartitionSpec as P

F32, BF16 = jnp.float32, jnp.bfloat16
LANES = 128
HALF = ("pr", "pl")
ALL = ("pr", "ph", "pl")
VMEM = pl.BlockSpec(memory_space=pltpu.VMEM)
HBM = pl.BlockSpec(memory_space=pltpu.HBM)


def dot(a, b, over_a, over_b):
    return lax.dot_general(a, b, (((over_a,), (over_b,)), ((), ())), preferred_element_type=F32)


def logistic(v):
    return 0.5 * jnp.tanh(0.5 * v) + 0.5


def params(limit=48 << 20):
    return pltpu.CompilerParams(vmem_limit_bytes=limit)


def cost(flops, nbytes):
    return pl.CostEstimate(flops=flops, bytes_accessed=nbytes, transcendentals=0)


def turned(*refs):
    return jnp.concatenate([r[...].astype(F32).T.astype(BF16) for r in refs], axis=0)


def factor_into(held_ref, rows, weights, take):
    width = weights.shape[0] // 2
    stride = held_ref.shape[0] // width

    def chunk(s, _):
        y = dot(weights, jnp.concatenate([take(2 * s), take(2 * s + 1)], axis=0), 1, 1)
        line = y[:width] * logistic(y[width:])
        for h in range(2):
            held_ref[pl.ds(2 * s + h, width, stride=stride), :] = line[:, h * LANES : (h + 1) * LANES]
        return 0

    lax.fori_loop(0, rows // 2, chunk, 0, unroll=8)


def lines_in(held_ref, first, count, rows, stride):
    held = held_ref[pl.ds(first * stride, count * stride), :].reshape(count, stride, LANES)
    return held[:, :rows].reshape(count * rows, LANES).astype(BF16)


def left_kernel(
    x_hbm, w_hbm, g_hbm, out_hbm, held_ref, wide_ref, x_ref, w_ref, g_ref, out_ref, sems, out_sems
):
    lines, ours = x_ref.shape[:2]
    pieces, step = sems.shape[0] - 2, ours + 8
    whole = [(w_hbm, w_ref), (g_hbm, g_ref)]
    for i in range(pieces):
        part = pl.ds(i * lines // pieces, lines // pieces)
        whole.append((x_hbm.at[part], x_ref.at[part]))
    copies = [pltpu.make_async_copy(a, b, sems.at[i]) for i, (a, b) in enumerate(whole)]
    for copy in copies[2:] + copies[:2]:
        copy.start()
    for i in range(pieces):
        copies[2 + i].wait()
        for k in range(i * lines // pieces, (i + 1) * lines // pieces):
            wide_ref[k * step : k * step + ours, :] = x_ref[k].astype(F32)
    parts = LANES // lines
    rows = ours // parts
    me = lax.axis_index("pr")
    first = [lax.rem(me + parts * t - t, parts) * rows for t in range(parts)]
    for copy in copies[:2]:
        copy.wait()
    weights = turned(w_ref), turned(g_ref)
    taken = [
        jnp.concatenate(
            [wide_ref[pl.ds(at + s, lines, stride=step), :] for at in first], axis=0
        ).astype(BF16)
        for s in range(rows)
    ]
    groups, ph = out_sems.shape
    pr, pc, size = out_ref.shape[:3]
    span = pr // groups
    count, stride = span * pc * size // rows, rows + 8
    copies = []
    for g in range(groups):
        mine = jnp.concatenate([w[g * count : (g + 1) * count] for w in weights], axis=0)
        for s in range(0, rows, 2):
            y = dot(mine, jnp.concatenate(taken[s : s + 2], axis=0), 1, 1)
            line = y[:count] * logistic(y[count:])
            for h in range(2):
                at = pl.ds(g * count * stride + s + h, count, stride=stride)
                held_ref[at, :] = line[:, h * LANES : (h + 1) * LANES]
        part = pl.ds(g * span, span)
        held = lines_in(held_ref, g * count, count, rows, stride)
        out_ref[part] = held.reshape(span, pc, size, LANES)
        for h in range(ph):
            copy = pltpu.make_async_copy(out_ref.at[part], out_hbm.at[part, h], out_sems.at[g, h])
            copy.start()
            copies.append(copy)
    for copy in copies:
        copy.wait()


def right_kernel(fold, x_ref, w_ref, g_ref, *rest):
    outs, held_ref = rest[:-1], rest[-1]
    rows = x_ref.shape[0] // fold

    def take(s):
        parts = [x_ref[e * rows + s] for e in range(fold)]
        return parts[0] if fold == 1 else jnp.concatenate(parts, axis=0)

    factor_into(held_ref, rows, turned(w_ref, g_ref), take)
    stride = rows + 8
    if len(outs) == 1:
        count = held_ref.shape[0] // stride
        outs[0][...] = lines_in(held_ref, 0, count, rows, stride).reshape(outs[0].shape)
    else:
        me = lax.axis_index(HALF)
        count = outs[0].shape[0] // rows
        for s, out in enumerate(outs):
            out[...] = lines_in(held_ref, (me ^ s) * count, count, rows, stride)


def gate_kernel(x_ref, og_ref, gain_ref, after_ref, gate_ref, gains_ref):
    lines, ours, depth = x_ref.shape

    def gate(k, _):
        x = x_ref[pl.ds(k * 2, 2)].reshape(2 * ours, depth)
        gate_ref[pl.ds(k * 2, 2)] = logistic(dot(x, og_ref[...], 1, 0)).reshape(2, ours, depth)
        return 0

    lax.fori_loop(0, lines // 2, gate, 0, unroll=2)
    gains_ref[...] = jnp.broadcast_to(gain_ref[...], (LANES, gain_ref.shape[1])).T


def slots(shape, count):
    return lax.broadcasted_iota(jnp.int32, shape, 1) // (LANES // count)


def pick(values):
    out = values[0]
    for t, value in enumerate(values[1:], 1):
        out = jnp.where(slots(out.shape, len(values)) == t, value, out)
    return out


def roll(value, by):
    by = by % LANES
    return value if by == 0 else pltpu.roll(value, by, 1)


def left_of(ref, ch, lines):
    pr, pc = ref.shape[:2]
    parts = LANES // lines
    bands = []
    for q in range(parts):
        tiles = []
        for g in range(0, pr, parts):
            cols = [
                roll(pick([ref[g + (t + q) % parts, c, ch] for t in range(parts)]), lines * q)
                for c in range(pc)
            ]
            tiles.append(jnp.concatenate(cols, axis=0))
        bands.append(jnp.concatenate(tiles, axis=1))
    return jnp.concatenate(bands, axis=0)


def right_of(get, pr, pc, fold):
    width = LANES // fold
    bands = []
    for p in range(pr):
        turns = [[roll(get(p, c), width * t) for t in range(fold)] for c in range(pc)]
        for e in range(fold):
            tiles = [pick([turn[(t - e) % fold] for t in range(fold)]) for turn in turns]
            bands.append(jnp.concatenate(tiles, axis=1))
    return jnp.concatenate(bands, axis=0)


def product_kernel(fold, scale, left_ref, after_ref, *rest):
    rights, out_ref, held = rest[:-2], *rest[-2:]
    rows_of, pc, channels, rows = out_ref.shape[:4]
    pr, blocks = left_ref.shape[:2]
    if len(rights) > 1:
        me = lax.axis_index(HALF)
        for s, right in enumerate(rights):
            held[me ^ s] = right[...]

    for ch in range(channels):
        left = left_of(left_ref, ch, rows * fold)
        if len(rights) > 1:
            at = slice(ch * rows, (ch + 1) * rows)
            right = right_of(lambda p, c: held[p * pc + c, at, :], pr, pc, fold)
        else:
            right = right_of(lambda p, c: rights[0][p, c, ch], pr, pc, fold)
        mixed = dot(left, right, 1, 0) * scale
        for p in range(rows_of):
            block, part = divmod(p, rows_of // blocks)
            at = [((part * fold + f) * blocks + block) * rows for f in range(fold)]
            for c in range(pc):
                lanes = slice(c * LANES, (c + 1) * LANES)
                out_ref[p, c, ch] = pick([mixed[a : a + rows, lanes] for a in at]).astype(BF16)


def pair_kernel(fold, mixed_ref, gate_ref, gains_ref, ow_ref, out_hbm, held_ref, out_ref, sems):
    depth, rows = mixed_ref.shape[:2]
    stride = rows + 1
    width = LANES // fold
    for d in range(depth):
        held_ref[d * stride : d * stride + rows, :] = mixed_ref[d].astype(F32)
    gain, weight = gains_ref[...], ow_ref[...]
    span = rows // sems.shape[0]
    copies = []
    for s in range(rows):
        v = held_ref[pl.ds(s, depth, stride=stride), :]
        centred = v - jnp.sum(v, axis=0, keepdims=True) * (1.0 / depth)
        spread = jnp.sum(centred * centred, axis=0, keepdims=True) * (1.0 / depth)
        scaled = (centred * lax.rsqrt(spread + 1e-05) * gain).astype(BF16)
        y = dot(scaled, weight, 0, 0)
        for f in range(fold):
            at = f * rows + s
            out_ref[at] = (y[f * width : (f + 1) * width] * gate_ref[at]).astype(BF16)
        if (s + 1) % span == 0:
            for f in range(fold):
                part = pl.ds(f * rows + s + 1 - span, span)
                copy = pltpu.make_async_copy(
                    out_ref.at[part], out_hbm.at[part], sems.at[s // span, f]
                )
                copy.start()
                copies.append(copy)
    for copy in copies:
        copy.wait()


def on_device(
    pair_array, left_weight, right_weight, left_gate, right_gate, mid_gain, out_weight, out_gate
):
    pr, ph, pc = lax.axis_size("pr"), lax.axis_size("ph"), lax.axis_size("pl")
    m = pr * pc
    lines, ours, depth = pair_array.shape
    mix = left_weight.shape[1]
    count = lines * pr
    fold = max(1, LANES // ours)
    rows = lines * ours // LANES
    channels = mix // m
    size = channels * rows
    hops = m <= 16 and m & (m - 1) == 0
    n_x = pair_array.size
    flops = 4 * lines * ours * depth * mix
    held = pltpu.VMEM((mix * (rows + 8), LANES), F32)

    left = pl.pallas_call(
        left_kernel,
        out_shape=jax.ShapeDtypeStruct((pr, ph, pc, size, LANES), BF16),
        in_specs=[HBM] * 3,
        out_specs=HBM,
        scratch_shapes=[
            held,
            pltpu.VMEM((lines * (ours + 8), depth), F32),
            *[pltpu.VMEM(a.shape, BF16) for a in (pair_array, left_weight, left_gate)],
            pltpu.VMEM((pr, pc, size, LANES), BF16),
            pltpu.SemaphoreType.DMA((4,)),
            pltpu.SemaphoreType.DMA((2, ph)),
        ],
        compiler_params=params(67043328),
        cost_estimate=cost(flops, 4 * n_x),
        name="left",
    )(pair_array, left_weight, left_gate)
    left = lax.all_to_all(left.reshape(pr * ph * pc, size, LANES), ALL, 0, 0, tiled=True)
    left = left.reshape(pr, ph * pc, channels, rows, LANES)

    if hops:
        shapes = [jax.ShapeDtypeStruct((size, LANES), BF16)] * m
    else:
        shapes = [jax.ShapeDtypeStruct((m, size, LANES), BF16)]
    right = pl.pallas_call(
        functools.partial(right_kernel, fold),
        out_shape=shapes,
        in_specs=[VMEM] * 3,
        out_specs=[VMEM] * len(shapes),
        scratch_shapes=[held],
        compiler_params=params(),
        cost_estimate=cost(flops, 4 * n_x),
        name="right",
    )(pair_array, right_weight, right_gate)
    gate, gains = pl.pallas_call(
        gate_kernel,
        out_shape=[
            jax.ShapeDtypeStruct(pair_array.shape, F32),
            jax.ShapeDtypeStruct((mix, LANES), F32),
        ],
        in_specs=[VMEM] * 4,
        out_specs=[VMEM] * 2,
        compiler_params=params(),
        cost_estimate=cost(flops // 2, 4 * n_x),
        name="gate",
    )(pair_array, out_gate, mid_gain.reshape(1, mix), right[0])
    if hops:
        right = list(right)
        for s in sorted(range(1, m), key=lambda s: s % pc == 0):
            right[s] = lax.ppermute(right[s], HALF, [(i, i ^ s) for i in range(m)])
    else:
        right = [lax.all_to_all(right[0], HALF, 0, 0, tiled=True)]
        right = [right[0].reshape(pr, pc, channels, rows, LANES)]

    if hops:
        at_once, blocks = channels, ph * pc
        right_specs = [pl.BlockSpec((size, LANES), lambda h, c: (0, 0))] * m
        kept = pltpu.VMEM((m, size, LANES), BF16)
    else:
        at_once, blocks = 1, 1
        right_specs = [
            pl.BlockSpec((pr, pc, at_once, rows, LANES), lambda h, c: (0, 0, h, 0, 0))
        ]
        kept = pltpu.VMEM((8, LANES), BF16)
    mixed = pl.pallas_call(
        functools.partial(product_kernel, fold, count ** (-0.5)),
        grid=(channels // at_once, ph * pc // blocks),
        out_shape=jax.ShapeDtypeStruct((pr, pc, channels, rows, LANES), BF16),
        in_specs=[
            pl.BlockSpec((pr, blocks, at_once, rows, LANES), lambda h, c: (0, c, h, 0, 0)),
            pl.BlockSpec((8, LANES), lambda h, c: (0, 0)),
            *right_specs,
        ],
        out_specs=pl.BlockSpec(
            (pr * blocks // (ph * pc), pc, at_once, rows, LANES), lambda h, c: (c, 0, h, 0, 0)
        ),
        scratch_shapes=[kept],
        compiler_params=params(),
        cost_estimate=cost(2 * count * count * ours * pc * channels, 8 * n_x),
        name="product",
    )(left, gains, *right)
    mixed = lax.all_to_all(mixed.reshape(m, size, LANES), HALF, 0, 0, tiled=True)
    return pl.pallas_call(
        functools.partial(pair_kernel, fold),
        out_shape=jax.ShapeDtypeStruct(pair_array.shape, BF16),
        in_specs=[VMEM] * 4,
        out_specs=HBM,
        scratch_shapes=[
            pltpu.VMEM((mix * (rows + 8), LANES), F32),
            pltpu.VMEM(pair_array.shape, BF16),
            pltpu.SemaphoreType.DMA((4, fold)),
        ],
        compiler_params=params(),
        cost_estimate=cost(flops // 2, 8 * n_x),
        name="pair",
    )(mixed.reshape(mix, rows, LANES), gate, gains, out_weight)


def solution(mesh):
    sizes = dict(mesh.shape)
    parts = 2 if sizes["pc"] % 2 == 0 else 1
    split = Mesh(mesh.devices.reshape(sizes["pr"], parts, sizes["pc"] // parts), ALL)
    spec = P("pr", ("ph", "pl"), None)
    return jax.shard_map(
        on_device,
        mesh=split,
        in_specs=(spec, P(), P(), P(), P(), P(), P(), P()),
        out_specs=spec,
        check_vma=False,
    )
```

```python
import functools

import jax
import jax.numpy as jnp
from jax import lax
from jax.experimental import pallas as pl
from jax.experimental.pallas import tpu as pltpu
from jax.sharding import Mesh, PartitionSpec as P

F32, BF16 = jnp.float32, jnp.bfloat16
LANES = 128
HALF = ("pr", "pl")
ALL = ("pr", "ph", "pl")
VMEM = pl.BlockSpec(memory_space=pltpu.VMEM)
HBM = pl.BlockSpec(memory_space=pltpu.HBM)


def dot(a, b, over_a, over_b):
    return lax.dot_general(a, b, (((over_a,), (over_b,)), ((), ())), preferred_element_type=F32)


def logistic(v):
    return 0.5 * jnp.tanh(0.5 * v) + 0.5


def params(limit=48 << 20):
    return pltpu.CompilerParams(vmem_limit_bytes=limit)


def cost(flops, nbytes):
    return pl.CostEstimate(flops=flops, bytes_accessed=nbytes, transcendentals=0)


def turned(*refs):
    return jnp.concatenate([r[...].astype(F32).T.astype(BF16) for r in refs], axis=0)


def factor_into(held_ref, rows, weights, take):
    width = weights.shape[0] // 2
    stride = held_ref.shape[0] // width

    def chunk(s, _):
        y = dot(weights, jnp.concatenate([take(2 * s), take(2 * s + 1)], axis=0), 1, 1)
        line = y[:width] * logistic(y[width:])
        for h in range(2):
            held_ref[pl.ds(2 * s + h, width, stride=stride), :] = line[:, h * LANES : (h + 1) * LANES]
        return 0

    lax.fori_loop(0, rows // 2, chunk, 0, unroll=8)


def lines_in(held_ref, first, count, rows, stride):
    held = held_ref[pl.ds(first * stride, count * stride), :].reshape(count, stride, LANES)
    return held[:, :rows].reshape(count * rows, LANES).astype(BF16)


def left_kernel(
    x_hbm, w_hbm, g_hbm, out_hbm, held_ref, wide_ref, x_ref, w_ref, g_ref, out_ref, sems, out_sems
):
    lines, ours = x_ref.shape[:2]
    pieces, step = sems.shape[0] - 2, ours + 8
    whole = [(w_hbm, w_ref), (g_hbm, g_ref)]
    for i in range(pieces):
        part = pl.ds(i * lines // pieces, lines // pieces)
        whole.append((x_hbm.at[part], x_ref.at[part]))
    copies = [pltpu.make_async_copy(a, b, sems.at[i]) for i, (a, b) in enumerate(whole)]
    for copy in copies[2:] + copies[:2]:
        copy.start()
    for i in range(pieces):
        copies[2 + i].wait()
        for k in range(i * lines // pieces, (i + 1) * lines // pieces):
            wide_ref[k * step : k * step + ours, :] = x_ref[k].astype(F32)
    parts = LANES // lines
    rows = ours // parts
    me = lax.axis_index("pr")
    first = [lax.rem(me + parts * t - t, parts) * rows for t in range(parts)]
    for copy in copies[:2]:
        copy.wait()
    weights = turned(w_ref), turned(g_ref)
    taken = [
        jnp.concatenate(
            [wide_ref[pl.ds(at + s, lines, stride=step), :] for at in first], axis=0
        ).astype(BF16)
        for s in range(rows)
    ]
    groups, ph = out_sems.shape
    pr, pc, size = out_ref.shape[:3]
    span = pr // groups
    count, stride = span * pc * size // rows, rows + 8
    copies = []
    for g in range(groups):
        mine = jnp.concatenate([w[g * count : (g + 1) * count] for w in weights], axis=0)
        for s in range(0, rows, 2):
            y = dot(mine, jnp.concatenate(taken[s : s + 2], axis=0), 1, 1)
            line = y[:count] * logistic(y[count:])
            for h in range(2):
                at = pl.ds(g * count * stride + s + h, count, stride=stride)
                held_ref[at, :] = line[:, h * LANES : (h + 1) * LANES]
        part = pl.ds(g * span, span)
        held = lines_in(held_ref, g * count, count, rows, stride)
        out_ref[part] = held.reshape(span, pc, size, LANES)
        for h in range(ph):
            copy = pltpu.make_async_copy(out_ref.at[part], out_hbm.at[part, h], out_sems.at[g, h])
            copy.start()
            copies.append(copy)
    for copy in copies:
        copy.wait()


def right_kernel(fold, x_ref, w_ref, g_ref, *rest):
    outs, held_ref = rest[:-1], rest[-1]
    rows = x_ref.shape[0] // fold

    def take(s):
        parts = [x_ref[e * rows + s] for e in range(fold)]
        return parts[0] if fold == 1 else jnp.concatenate(parts, axis=0)

    factor_into(held_ref, rows, turned(w_ref, g_ref), take)
    stride = rows + 8
    if len(outs) == 1:
        count = held_ref.shape[0] // stride
        outs[0][...] = lines_in(held_ref, 0, count, rows, stride).reshape(outs[0].shape)
    else:
        me = lax.axis_index(HALF)
        count = outs[0].shape[0] // rows
        for s, out in enumerate(outs):
            out[...] = lines_in(held_ref, (me ^ s) * count, count, rows, stride)


def gate_kernel(x_ref, og_ref, gain_ref, after_ref, gate_ref, gains_ref):
    lines, ours, depth = x_ref.shape

    def gate(k, _):
        x = x_ref[pl.ds(k * 2, 2)].reshape(2 * ours, depth)
        gate_ref[pl.ds(k * 2, 2)] = logistic(dot(x, og_ref[...], 1, 0)).reshape(2, ours, depth)
        return 0

    lax.fori_loop(0, lines // 2, gate, 0, unroll=2)
    gains_ref[...] = jnp.broadcast_to(gain_ref[...], (LANES, gain_ref.shape[1])).T


def slots(shape, count):
    return lax.broadcasted_iota(jnp.int32, shape, 1) // (LANES // count)


def pick(values):
    out = values[0]
    for t, value in enumerate(values[1:], 1):
        out = jnp.where(slots(out.shape, len(values)) == t, value, out)
    return out


def roll(value, by):
    by = by % LANES
    return value if by == 0 else pltpu.roll(value, by, 1)


def left_of(ref, ch, lines):
    pr, pc = ref.shape[:2]
    parts = LANES // lines
    bands = []
    for q in range(parts):
        tiles = []
        for g in range(0, pr, parts):
            cols = [
                roll(pick([ref[g + (t + q) % parts, c, ch] for t in range(parts)]), lines * q)
                for c in range(pc)
            ]
            tiles.append(jnp.concatenate(cols, axis=0))
        bands.append(jnp.concatenate(tiles, axis=1))
    return jnp.concatenate(bands, axis=0)


def right_of(get, pr, pc, fold):
    width = LANES // fold
    bands = []
    for p in range(pr):
        turns = [[roll(get(p, c), width * t) for t in range(fold)] for c in range(pc)]
        for e in range(fold):
            tiles = [pick([turn[(t - e) % fold] for t in range(fold)]) for turn in turns]
            bands.append(jnp.concatenate(tiles, axis=1))
    return jnp.concatenate(bands, axis=0)


def product_kernel(fold, scale, left_ref, after_ref, *rest):
    rights, out_ref, held = rest[:-2], *rest[-2:]
    rows_of, pc, channels, rows = out_ref.shape[:4]
    pr, blocks = left_ref.shape[:2]
    if len(rights) > 1:
        me = lax.axis_index(HALF)
        for s, right in enumerate(rights):
            held[me ^ s] = right[...]

    for ch in range(channels):
        left = left_of(left_ref, ch, rows * fold)
        if len(rights) > 1:
            at = slice(ch * rows, (ch + 1) * rows)
            right = right_of(lambda p, c: held[p * pc + c, at, :], pr, pc, fold)
        else:
            right = right_of(lambda p, c: rights[0][p, c, ch], pr, pc, fold)
        mixed = dot(left, right, 1, 0) * scale
        for p in range(rows_of):
            block, part = divmod(p, rows_of // blocks)
            at = [((part * fold + f) * blocks + block) * rows for f in range(fold)]
            for c in range(pc):
                lanes = slice(c * LANES, (c + 1) * LANES)
                out_ref[p, c, ch] = pick([mixed[a : a + rows, lanes] for a in at]).astype(BF16)


def pair_kernel(fold, mixed_ref, gate_ref, gains_ref, ow_ref, out_hbm, held_ref, out_ref, sems):
    depth, rows = mixed_ref.shape[:2]
    stride = rows + 1
    width = LANES // fold
    for d in range(depth):
        held_ref[d * stride : d * stride + rows, :] = mixed_ref[d].astype(F32)
    gain, weight = gains_ref[...], ow_ref[...]
    span = rows // sems.shape[0]
    copies = []
    for s in range(rows):
        v = held_ref[pl.ds(s, depth, stride=stride), :]
        centred = v - jnp.sum(v, axis=0, keepdims=True) * (1.0 / depth)
        spread = jnp.sum(centred * centred, axis=0, keepdims=True) * (1.0 / depth)
        scaled = (centred * lax.rsqrt(spread + 1e-05) * gain).astype(BF16)
        y = dot(scaled, weight, 0, 0)
        for f in range(fold):
            at = f * rows + s
            out_ref[at] = (y[f * width : (f + 1) * width] * gate_ref[at]).astype(BF16)
        done = s if s % span == 0 else rows if s == rows - 1 else 0
        for f in range(fold if done else 0):
            part = pl.ds(f * rows + done - span, span)
            copy = pltpu.make_async_copy(
                out_ref.at[part], out_hbm.at[part], sems.at[done // span - 1, f]
            )
            copy.start()
            copies.append(copy)
    for copy in copies:
        copy.wait()


def on_device(
    pair_array, left_weight, right_weight, left_gate, right_gate, mid_gain, out_weight, out_gate
):
    pr, ph, pc = lax.axis_size("pr"), lax.axis_size("ph"), lax.axis_size("pl")
    m = pr * pc
    lines, ours, depth = pair_array.shape
    mix = left_weight.shape[1]
    count = lines * pr
    fold = max(1, LANES // ours)
    rows = lines * ours // LANES
    channels = mix // m
    size = channels * rows
    hops = m <= 16 and m & (m - 1) == 0
    n_x = pair_array.size
    flops = 4 * lines * ours * depth * mix
    held = pltpu.VMEM((mix * (rows + 8), LANES), F32)

    left = pl.pallas_call(
        left_kernel,
        out_shape=jax.ShapeDtypeStruct((pr, ph, pc, size, LANES), BF16),
        in_specs=[HBM] * 3,
        out_specs=HBM,
        scratch_shapes=[
            held,
            pltpu.VMEM((lines * (ours + 8), depth), F32),
            *[pltpu.VMEM(a.shape, BF16) for a in (pair_array, left_weight, left_gate)],
            pltpu.VMEM((pr, pc, size, LANES), BF16),
            pltpu.SemaphoreType.DMA((4,)),
            pltpu.SemaphoreType.DMA((2, ph)),
        ],
        compiler_params=params(67043328),
        cost_estimate=cost(flops, 4 * n_x),
        name="left",
    )(pair_array, left_weight, left_gate)
    left = lax.all_to_all(left.reshape(pr * ph * pc, size, LANES), ALL, 0, 0, tiled=True)
    left = left.reshape(pr, ph * pc, channels, rows, LANES)

    if hops:
        shapes = [jax.ShapeDtypeStruct((size, LANES), BF16)] * m
    else:
        shapes = [jax.ShapeDtypeStruct((m, size, LANES), BF16)]
    right = pl.pallas_call(
        functools.partial(right_kernel, fold),
        out_shape=shapes,
        in_specs=[VMEM] * 3,
        out_specs=[VMEM] * len(shapes),
        scratch_shapes=[held],
        compiler_params=params(),
        cost_estimate=cost(flops, 4 * n_x),
        name="right",
    )(pair_array, right_weight, right_gate)
    gate, gains = pl.pallas_call(
        gate_kernel,
        out_shape=[
            jax.ShapeDtypeStruct(pair_array.shape, F32),
            jax.ShapeDtypeStruct((mix, LANES), F32),
        ],
        in_specs=[VMEM] * 4,
        out_specs=[VMEM] * 2,
        compiler_params=params(),
        cost_estimate=cost(flops // 2, 4 * n_x),
        name="gate",
    )(pair_array, out_gate, mid_gain.reshape(1, mix), right[0])
    if hops:
        right = list(right)
        for s in sorted(range(1, m), key=lambda s: s % pc == 0):
            right[s] = lax.ppermute(right[s], HALF, [(i, i ^ s) for i in range(m)])
    else:
        right = [lax.all_to_all(right[0], HALF, 0, 0, tiled=True)]
        right = [right[0].reshape(pr, pc, channels, rows, LANES)]

    if hops:
        at_once, blocks = channels, ph * pc
        right_specs = [pl.BlockSpec((size, LANES), lambda h, c: (0, 0))] * m
        kept = pltpu.VMEM((m, size, LANES), BF16)
    else:
        at_once, blocks = 1, 1
        right_specs = [
            pl.BlockSpec((pr, pc, at_once, rows, LANES), lambda h, c: (0, 0, h, 0, 0))
        ]
        kept = pltpu.VMEM((8, LANES), BF16)
    mixed = pl.pallas_call(
        functools.partial(product_kernel, fold, count ** (-0.5)),
        grid=(channels // at_once, ph * pc // blocks),
        out_shape=jax.ShapeDtypeStruct((pr, pc, channels, rows, LANES), BF16),
        in_specs=[
            pl.BlockSpec((pr, blocks, at_once, rows, LANES), lambda h, c: (0, c, h, 0, 0)),
            pl.BlockSpec((8, LANES), lambda h, c: (0, 0)),
            *right_specs,
        ],
        out_specs=pl.BlockSpec(
            (pr * blocks // (ph * pc), pc, at_once, rows, LANES), lambda h, c: (c, 0, h, 0, 0)
        ),
        scratch_shapes=[kept],
        compiler_params=params(),
        cost_estimate=cost(2 * count * count * ours * pc * channels, 8 * n_x),
        name="product",
    )(left, gains, *right)
    mixed = lax.all_to_all(mixed.reshape(m, size, LANES), HALF, 0, 0, tiled=True)
    return pl.pallas_call(
        functools.partial(pair_kernel, fold),
        out_shape=jax.ShapeDtypeStruct(pair_array.shape, BF16),
        in_specs=[VMEM] * 4,
        out_specs=HBM,
        scratch_shapes=[
            pltpu.VMEM((mix * (rows + 8), LANES), F32),
            pltpu.VMEM(pair_array.shape, BF16),
            pltpu.SemaphoreType.DMA((4, fold)),
        ],
        compiler_params=params(),
        cost_estimate=cost(flops // 2, 8 * n_x),
        name="pair",
    )(mixed.reshape(mix, rows, LANES), gate, gains, out_weight)


def solution(mesh):
    sizes = dict(mesh.shape)
    parts = 2 if sizes["pc"] % 2 == 0 else 1
    split = Mesh(mesh.devices.reshape(sizes["pr"], parts, sizes["pc"] // parts), ALL)
    spec = P("pr", ("ph", "pl"), None)
    return jax.shard_map(
        on_device,
        mesh=split,
        in_specs=(spec, P(), P(), P(), P(), P(), P(), P()),
        out_specs=spec,
        check_vma=False,
    )
```

```python
import functools

import jax
import jax.numpy as jnp
from jax import lax
from jax.experimental import pallas as pl
from jax.experimental.pallas import tpu as pltpu
from jax.sharding import Mesh, PartitionSpec as P

F32, BF16 = jnp.float32, jnp.bfloat16
LANES = 128
HALF = ("pr", "pl")
ALL = ("pr", "ph", "pl")
VMEM = pl.BlockSpec(memory_space=pltpu.VMEM)
HBM = pl.BlockSpec(memory_space=pltpu.HBM)


def dot(a, b, over_a, over_b):
    return lax.dot_general(a, b, (((over_a,), (over_b,)), ((), ())), preferred_element_type=F32)


def logistic(v):
    return 0.5 * jnp.tanh(0.5 * v) + 0.5


def params(limit=48 << 20):
    return pltpu.CompilerParams(vmem_limit_bytes=limit)


def cost(flops, nbytes):
    return pl.CostEstimate(flops=flops, bytes_accessed=nbytes, transcendentals=0)


def turned(*refs):
    return jnp.concatenate([r[...].astype(F32).T.astype(BF16) for r in refs], axis=0)


def factor_into(held_ref, rows, weights, take):
    width = weights.shape[0] // 2
    stride = held_ref.shape[0] // width

    def chunk(s, _):
        y = dot(weights, jnp.concatenate([take(2 * s), take(2 * s + 1)], axis=0), 1, 1)
        line = y[:width] * logistic(y[width:])
        for h in range(2):
            held_ref[pl.ds(2 * s + h, width, stride=stride), :] = line[:, h * LANES : (h + 1) * LANES]
        return 0

    lax.fori_loop(0, rows // 2, chunk, 0, unroll=8)


def lines_in(held_ref, first, count, rows, stride):
    held = held_ref[pl.ds(first * stride, count * stride), :].reshape(count, stride, LANES)
    return held[:, :rows].reshape(count * rows, LANES).astype(BF16)


def left_kernel(
    x_hbm, w_hbm, g_hbm, out_hbm, held_ref, wide_ref, x_ref, w_ref, g_ref, out_ref, sems, out_sems
):
    lines, ours = x_ref.shape[:2]
    pieces, step = sems.shape[0] - 2, ours + 8
    whole = [(w_hbm, w_ref), (g_hbm, g_ref)]
    for i in range(pieces):
        part = pl.ds(i * lines // pieces, lines // pieces)
        whole.append((x_hbm.at[part], x_ref.at[part]))
    copies = [pltpu.make_async_copy(a, b, sems.at[i]) for i, (a, b) in enumerate(whole)]
    for copy in copies[2:] + copies[:2]:
        copy.start()
    for i in range(pieces):
        copies[2 + i].wait()
        for k in range(i * lines // pieces, (i + 1) * lines // pieces):
            wide_ref[k * step : k * step + ours, :] = x_ref[k].astype(F32)
    parts = LANES // lines
    rows = ours // parts
    me = lax.axis_index("pr")
    first = [lax.rem(me + parts * t - t, parts) * rows for t in range(parts)]
    for copy in copies[:2]:
        copy.wait()
    weights = turned(w_ref), turned(g_ref)
    taken = [
        jnp.concatenate(
            [wide_ref[pl.ds(at + s, lines, stride=step), :] for at in first], axis=0
        ).astype(BF16)
        for s in range(rows)
    ]
    groups, ph = out_sems.shape
    pr, pc, size = out_ref.shape[:3]
    span = pr // groups
    count, stride = span * pc * size // rows, rows + 8
    copies = []
    for g in range(groups):
        mine = jnp.concatenate([w[g * count : (g + 1) * count] for w in weights], axis=0)
        for s in range(0, rows, 2):
            if s == 2 and g > 0:
                for copy in copies[ph * (g - 1) :]:
                    copy.start()
            y = dot(mine, jnp.concatenate(taken[s : s + 2], axis=0), 1, 1)
            line = y[:count] * logistic(y[count:])
            for h in range(2):
                at = pl.ds(g * count * stride + s + h, count, stride=stride)
                held_ref[at, :] = line[:, h * LANES : (h + 1) * LANES]
        part = pl.ds(g * span, span)
        held = lines_in(held_ref, g * count, count, rows, stride)
        out_ref[part] = held.reshape(span, pc, size, LANES)
        for h in range(ph):
            copies.append(
                pltpu.make_async_copy(out_ref.at[part], out_hbm.at[part, h], out_sems.at[g, h])
            )
    for copy in copies[ph * (groups - 1) :]:
        copy.start()
    for copy in copies:
        copy.wait()


def right_kernel(fold, x_ref, w_ref, g_ref, *rest):
    outs, held_ref = rest[:-1], rest[-1]
    rows = x_ref.shape[0] // fold

    def take(s):
        parts = [x_ref[e * rows + s] for e in range(fold)]
        return parts[0] if fold == 1 else jnp.concatenate(parts, axis=0)

    factor_into(held_ref, rows, turned(w_ref, g_ref), take)
    stride = rows + 8
    if len(outs) == 1:
        count = held_ref.shape[0] // stride
        outs[0][...] = lines_in(held_ref, 0, count, rows, stride).reshape(outs[0].shape)
    else:
        me = lax.axis_index(HALF)
        count = outs[0].shape[0] // rows
        for s, out in enumerate(outs):
            out[...] = lines_in(held_ref, (me ^ s) * count, count, rows, stride)


def gate_kernel(x_ref, og_ref, gain_ref, after_ref, gate_ref, gains_ref):
    lines, ours, depth = x_ref.shape

    def gate(k, _):
        x = x_ref[pl.ds(k * 2, 2)].reshape(2 * ours, depth)
        gate_ref[pl.ds(k * 2, 2)] = logistic(dot(x, og_ref[...], 1, 0)).reshape(2, ours, depth)
        return 0

    lax.fori_loop(0, lines // 2, gate, 0, unroll=2)
    gains_ref[...] = jnp.broadcast_to(gain_ref[...], (LANES, gain_ref.shape[1])).T


def slots(shape, count):
    return lax.broadcasted_iota(jnp.int32, shape, 1) // (LANES // count)


def pick(values):
    out = values[0]
    for t, value in enumerate(values[1:], 1):
        out = jnp.where(slots(out.shape, len(values)) == t, value, out)
    return out


def roll(value, by):
    by = by % LANES
    return value if by == 0 else pltpu.roll(value, by, 1)


def left_of(ref, ch, lines):
    pr, pc = ref.shape[:2]
    parts = LANES // lines
    bands = []
    for q in range(parts):
        tiles = []
        for g in range(0, pr, parts):
            cols = [
                roll(pick([ref[g + (t + q) % parts, c, ch] for t in range(parts)]), lines * q)
                for c in range(pc)
            ]
            tiles.append(jnp.concatenate(cols, axis=0))
        bands.append(jnp.concatenate(tiles, axis=1))
    return jnp.concatenate(bands, axis=0)


def right_of(get, pr, pc, fold):
    width = LANES // fold
    bands = []
    for p in range(pr):
        turns = [[roll(get(p, c), width * t) for t in range(fold)] for c in range(pc)]
        for e in range(fold):
            tiles = [pick([turn[(t - e) % fold] for t in range(fold)]) for turn in turns]
            bands.append(jnp.concatenate(tiles, axis=1))
    return jnp.concatenate(bands, axis=0)


def product_kernel(fold, scale, left_ref, after_ref, *rest):
    rights, out_ref, held = rest[:-2], *rest[-2:]
    rows_of, pc, channels, rows = out_ref.shape[:4]
    pr, blocks = left_ref.shape[:2]
    if len(rights) > 1:
        me = lax.axis_index(HALF)
        for s, right in enumerate(rights):
            held[me ^ s] = right[...]

    for ch in range(channels):
        left = left_of(left_ref, ch, rows * fold)
        if len(rights) > 1:
            at = slice(ch * rows, (ch + 1) * rows)
            right = right_of(lambda p, c: held[p * pc + c, at, :], pr, pc, fold)
        else:
            right = right_of(lambda p, c: rights[0][p, c, ch], pr, pc, fold)
        mixed = dot(left, right, 1, 0) * scale
        for p in range(rows_of):
            block, part = divmod(p, rows_of // blocks)
            at = [((part * fold + f) * blocks + block) * rows for f in range(fold)]
            for c in range(pc):
                lanes = slice(c * LANES, (c + 1) * LANES)
                out_ref[p, c, ch] = pick([mixed[a : a + rows, lanes] for a in at]).astype(BF16)


def pair_kernel(fold, mixed_ref, gate_ref, gains_ref, ow_ref, out_hbm, held_ref, out_ref, sems):
    depth, rows = mixed_ref.shape[:2]
    stride = rows + 1
    width = LANES // fold
    for d in range(depth):
        held_ref[d * stride : d * stride + rows, :] = mixed_ref[d].astype(F32)
    gain, weight = gains_ref[...], ow_ref[...]
    span = rows // sems.shape[0]
    copies = []
    for s in range(rows):
        v = held_ref[pl.ds(s, depth, stride=stride), :]
        centred = v - jnp.sum(v, axis=0, keepdims=True) * (1.0 / depth)
        spread = jnp.sum(centred * centred, axis=0, keepdims=True) * (1.0 / depth)
        scaled = (centred * lax.rsqrt(spread + 1e-05) * gain).astype(BF16)
        y = dot(scaled, weight, 0, 0)
        for f in range(fold):
            at = f * rows + s
            out_ref[at] = (y[f * width : (f + 1) * width] * gate_ref[at]).astype(BF16)
        done = s if s % span == 0 else rows if s == rows - 1 else 0
        for f in range(fold if done else 0):
            part = pl.ds(f * rows + done - span, span)
            copy = pltpu.make_async_copy(
                out_ref.at[part], out_hbm.at[part], sems.at[done // span - 1, f]
            )
            copy.start()
            copies.append(copy)
    for copy in copies:
        copy.wait()


def on_device(
    pair_array, left_weight, right_weight, left_gate, right_gate, mid_gain, out_weight, out_gate
):
    pr, ph, pc = lax.axis_size("pr"), lax.axis_size("ph"), lax.axis_size("pl")
    m = pr * pc
    lines, ours, depth = pair_array.shape
    mix = left_weight.shape[1]
    count = lines * pr
    fold = max(1, LANES // ours)
    rows = lines * ours // LANES
    channels = mix // m
    size = channels * rows
    hops = m <= 16 and m & (m - 1) == 0
    n_x = pair_array.size
    flops = 4 * lines * ours * depth * mix
    held = pltpu.VMEM((mix * (rows + 8), LANES), F32)

    left = pl.pallas_call(
        left_kernel,
        out_shape=jax.ShapeDtypeStruct((pr, ph, pc, size, LANES), BF16),
        in_specs=[HBM] * 3,
        out_specs=HBM,
        scratch_shapes=[
            held,
            pltpu.VMEM((lines * (ours + 8), depth), F32),
            *[pltpu.VMEM(a.shape, BF16) for a in (pair_array, left_weight, left_gate)],
            pltpu.VMEM((pr, pc, size, LANES), BF16),
            pltpu.SemaphoreType.DMA((4,)),
            pltpu.SemaphoreType.DMA((2, ph)),
        ],
        compiler_params=params(67043328),
        cost_estimate=cost(flops, 4 * n_x),
        name="left",
    )(pair_array, left_weight, left_gate)
    left = lax.all_to_all(left.reshape(pr * ph * pc, size, LANES), ALL, 0, 0, tiled=True)
    left = left.reshape(pr, ph * pc, channels, rows, LANES)

    if hops:
        shapes = [jax.ShapeDtypeStruct((size, LANES), BF16)] * m
    else:
        shapes = [jax.ShapeDtypeStruct((m, size, LANES), BF16)]
    right = pl.pallas_call(
        functools.partial(right_kernel, fold),
        out_shape=shapes,
        in_specs=[VMEM] * 3,
        out_specs=[VMEM] * len(shapes),
        scratch_shapes=[held],
        compiler_params=params(),
        cost_estimate=cost(flops, 4 * n_x),
        name="right",
    )(pair_array, right_weight, right_gate)
    gate, gains = pl.pallas_call(
        gate_kernel,
        out_shape=[
            jax.ShapeDtypeStruct(pair_array.shape, F32),
            jax.ShapeDtypeStruct((mix, LANES), F32),
        ],
        in_specs=[VMEM] * 4,
        out_specs=[VMEM] * 2,
        compiler_params=params(),
        cost_estimate=cost(flops // 2, 4 * n_x),
        name="gate",
    )(pair_array, out_gate, mid_gain.reshape(1, mix), right[0])
    if hops:
        right = list(right)
        for s in sorted(range(1, m), key=lambda s: s % pc == 0):
            right[s] = lax.ppermute(right[s], HALF, [(i, i ^ s) for i in range(m)])
    else:
        right = [lax.all_to_all(right[0], HALF, 0, 0, tiled=True)]
        right = [right[0].reshape(pr, pc, channels, rows, LANES)]

    if hops:
        at_once, blocks = channels, ph * pc
        right_specs = [pl.BlockSpec((size, LANES), lambda h, c: (0, 0))] * m
        kept = pltpu.VMEM((m, size, LANES), BF16)
    else:
        at_once, blocks = 1, 1
        right_specs = [
            pl.BlockSpec((pr, pc, at_once, rows, LANES), lambda h, c: (0, 0, h, 0, 0))
        ]
        kept = pltpu.VMEM((8, LANES), BF16)
    mixed = pl.pallas_call(
        functools.partial(product_kernel, fold, count ** (-0.5)),
        grid=(channels // at_once, ph * pc // blocks),
        out_shape=jax.ShapeDtypeStruct((pr, pc, channels, rows, LANES), BF16),
        in_specs=[
            pl.BlockSpec((pr, blocks, at_once, rows, LANES), lambda h, c: (0, c, h, 0, 0)),
            pl.BlockSpec((8, LANES), lambda h, c: (0, 0)),
            *right_specs,
        ],
        out_specs=pl.BlockSpec(
            (pr * blocks // (ph * pc), pc, at_once, rows, LANES), lambda h, c: (c, 0, h, 0, 0)
        ),
        scratch_shapes=[kept],
        compiler_params=params(),
        cost_estimate=cost(2 * count * count * ours * pc * channels, 8 * n_x),
        name="product",
    )(left, gains, *right)
    mixed = lax.all_to_all(mixed.reshape(m, size, LANES), HALF, 0, 0, tiled=True)
    return pl.pallas_call(
        functools.partial(pair_kernel, fold),
        out_shape=jax.ShapeDtypeStruct(pair_array.shape, BF16),
        in_specs=[VMEM] * 4,
        out_specs=HBM,
        scratch_shapes=[
            pltpu.VMEM((mix * (rows + 8), LANES), F32),
            pltpu.VMEM(pair_array.shape, BF16),
            pltpu.SemaphoreType.DMA((4, fold)),
        ],
        compiler_params=params(),
        cost_estimate=cost(flops // 2, 8 * n_x),
        name="pair",
    )(mixed.reshape(mix, rows, LANES), gate, gains, out_weight)


def solution(mesh):
    sizes = dict(mesh.shape)
    parts = 2 if sizes["pc"] % 2 == 0 else 1
    split = Mesh(mesh.devices.reshape(sizes["pr"], parts, sizes["pc"] // parts), ALL)
    spec = P("pr", ("ph", "pl"), None)
    return jax.shard_map(
        on_device,
        mesh=split,
        in_specs=(spec, P(), P(), P(), P(), P(), P(), P()),
        out_specs=spec,
        check_vma=False,
    )
```
